32 devices in a mesh: grp: 4 (over x, core), sub: 8 (over z, y).
Axes of the slice: x: 2, y: 2, z: 4, core: 2. Of those that a mesh axis runs over, the one named last changes fastest.
Arguments:
- fine_res: float32 [3, 131072], P(None, ('grp', 'sub'))
- node_map: int32 [2, 131072], P(None, ('grp', 'sub')), may hold values from 0 to 16383, as said below
- connect: int32 [4, 32768], P(None, 'sub'), may hold values from 0 to 16383, as said below
- grads: float32 [3, 3, 32768], P(None, None, 'sub'), may hold values from -6 to 6
- moduli: float32 [2, 32768], P(None, 'sub'), may hold values from 0.2 to 2
- mass: float32 [16384], P('sub'), may hold values from 0.5 to 4
Outputs:
- correction: float32 [3, 131072], P(None, ('grp', 'sub'))
The draws below stay inside these ranges and needn't reach their ends.
Inputs may be any that keep to these rules, and one draw needn't show every extreme that they name: `node_map`: fine nodes 4096 * b to 4096 * (b + 1) - 1 lie in column c = b % 8; both their entries are coarse nodes c * 2048 to (c + 1) * 2048 - 1 or the first 1024 nodes of column c + 1; the two entries are equal at vertices. `connect`: tetrahedra c * 4096 to (c + 1) * 4096 - 1 lie in column c; their nodes are coarse nodes of column c or the first 1024 nodes of column c + 1.
All inputs are finite; a program needn't handle non-finite values.
Results may differ from the reference program's by a relative error of at most 0.0001.
Values sent between devices are 32-bit elements; how exact they have to be, the bound alone decides.
No kernel may reach another device: no remote copies, remote signals or barrier semaphores. Data moves between devices by JAX's collectives and lax.ppermute only.
A program may use at most 64 MiB of HBM per device.

```python
import math
import jax
import jax.numpy as jnp

CN = 2048
CI = 1024
CE = 4096
FN = 4096
ITERS = 3
CNODES = 16384
CELEMS = 32768
FNODES = 131072
N_SUB = 8


def pick_nodes(key, count, column):
    keys = jax.random.split(key, 3)
    own = jax.random.randint(keys[0], (count,), 0, CN, dtype=jnp.int32)
    shared = jax.random.randint(keys[1], (count,), 0, CI, dtype=jnp.int32)
    coin = jax.random.randint(keys[2], (count,), 0, 100, dtype=jnp.int32)
    use_next = (coin < 20) & (column < N_SUB - 1)
    return jnp.where(use_next, (column + 1) * CN + shared, column * CN + own).astype(jnp.int32)


def draw_fine_res(key, part):
    column = jnp.arange(FNODES, dtype=jnp.int32) // FN % N_SUB
    scale = 1.0 + 2.0 * column.astype(jnp.float32) / max(N_SUB - 1, 1)
    values = jax.random.normal(key, (3, FNODES), jnp.float32) * scale[None, :]
    return values


def draw_node_map(key, part):
    column = jnp.arange(FNODES, dtype=jnp.int32) // FN % N_SUB
    keys = jax.random.split(jax.random.fold_in(key, 11), 3)
    first = pick_nodes(keys[0], FNODES, column)
    second = pick_nodes(keys[1], FNODES, column)
    coin = jax.random.randint(keys[2], (FNODES,), 0, 8, dtype=jnp.int32)
    second = jnp.where(coin == 0, first, second)
    return jnp.stack([first, second]).astype(jnp.int32)


def draw_connect(key, part):
    column = jnp.arange(CELEMS, dtype=jnp.int32) // CE
    keys = jax.random.split(jax.random.fold_in(key, 23), 4)
    return jnp.stack([pick_nodes(keys[corner], CELEMS, column) for corner in range(4)]).astype(jnp.int32)


def block_levels(own_key, extent, cuts, low, largest):
    gain, own = 1.0, jax.random.fold_in(own_key, 6)
    for axis_at, shards_of in cuts:
        draws = jnp.exp(jax.random.uniform(jax.random.fold_in(own, axis_at), (shards_of,), jnp.float32, low / len(cuts), largest / len(cuts)))
        gain = gain * jnp.repeat(draws, extent[axis_at] // shards_of).reshape([-1 if axis == axis_at else 1 for axis in range(len(extent))])
    return gain


def normal_values(key, shape, spread, most, shards=(), held_as=jnp.bfloat16):
    drawn = jax.random.normal(key, shape, jnp.float32) * spread
    if len(shards) > 0:
        drawn = block_levels(key, shape, shards, -0.22, 0.18) * drawn
    return jnp.clip(drawn, min=-most, max=most).astype(held_as)


def setup_inputs(seed: int = 0) -> dict:
    streams_of = jax.random.split(jax.random.key(seed), 7)
    fine_res = draw_fine_res(jax.random.fold_in(streams_of[6], 71), 0)
    node_map = draw_node_map(jax.random.fold_in(streams_of[6], 71), 0)
    connect = draw_connect(jax.random.fold_in(streams_of[6], 71), 0)
    grads = normal_values(streams_of[3], (3, 3, CELEMS), 1.0, 6.0, ((2, 8),), jnp.float32)
    moduli = jnp.clip(jnp.exp(math.log(2.0) - 2.3025851 * jax.random.uniform(streams_of[4], (2, CELEMS), jnp.float32) ** block_levels(streams_of[4], (2, CELEMS), ((1, 8),), -0.2, 0.2)), 0.2, 2.0)
    mass = jnp.clip(jnp.exp(math.log(4.0) - 2.0794415 * jax.random.uniform(streams_of[5], (CNODES,), jnp.float32) ** block_levels(streams_of[5], (CNODES,), ((0, 8),), -0.2, 0.2)), 0.5, 4.0)
    return {"fine_res": fine_res, "node_map": node_map, "connect": connect, "grads": grads, "moduli": moduli, "mass": mass}


def element_forces(field, connect, grads, moduli, count):
    last = -(grads[:, 0] + grads[:, 1] + grads[:, 2])
    shape_grads = (grads[:, 0], grads[:, 1], grads[:, 2], last)
    displ_grad = jnp.zeros((3, 3, connect.shape[1]), jnp.float32)
    for corner in range(4):
        moved = jnp.take(field, connect[corner], axis=1)
        displ_grad = displ_grad + moved[:, None, :] * shape_grads[corner][None, :, :]
    strain = 0.5 * (displ_grad + jnp.transpose(displ_grad, (1, 0, 2)))
    trace = strain[0, 0] + strain[1, 1] + strain[2, 2]
    identity = jnp.eye(3, dtype=jnp.float32)[:, :, None]
    stress = 2.0 * moduli[1] * strain + (moduli[0] * trace) * identity
    forces = jnp.zeros((3, count), jnp.float32)
    for corner in range(4):
        nodal = jnp.sum(stress * shape_grads[corner][None, :, :], axis=1)
        forces = forces.at[:, connect[corner]].add(nodal)
    return forces


def operate(field, connect, grads, moduli, mass):
    return mass[None, :] * field + element_forces(field, connect, grads, moduli, field.shape[1])


def reference(fine_res, node_map, connect, grads, moduli, mass):
    total = mass.shape[0]
    half = 0.5 * fine_res
    rhs = jnp.zeros((3, total), jnp.float32).at[:, node_map[0]].add(half).at[:, node_map[1]].add(half)
    solution = jnp.zeros((3, total), jnp.float32)
    residual = rhs
    direction = rhs
    norm_now = jnp.sum(residual * residual)
    for step in range(ITERS):
        image = operate(direction, connect, grads, moduli, mass)
        alpha = norm_now / jnp.sum(direction * image)
        solution = solution + alpha * direction
        residual = residual - alpha * image
        norm_next = jnp.sum(residual * residual)
        direction = residual + (norm_next / norm_now) * direction
        norm_now = norm_next
    return 0.5 * (jnp.take(solution, node_map[0], axis=1) + jnp.take(solution, node_map[1], axis=1))
```

```python
import functools

import jax
import jax.numpy as jnp
from jax import lax
from jax.experimental import pallas as pl
from jax.experimental.pallas import tpu as pltpu
from jax.sharding import PartitionSpec as P

CI = 1024
LANE = 128
LO = 256
HP = 16
RC = 8


def split3(x):
    a = x.astype(jnp.bfloat16).astype(jnp.float32)
    r = x - a
    b = r.astype(jnp.bfloat16).astype(jnp.float32)
    return a, b, r - b


def gather(table, idxs, rows):
    lo = [i & (LANE - 1) for i in idxs]
    hi = [i >> 7 for i in idxs]
    out = [[jnp.zeros((8, LANE), jnp.float32)] * 3 for _ in idxs]
    for h in range(rows * LO // LANE):
        r, half = divmod(h, LO // LANE)
        cols = slice(half * LANE, (half + 1) * LANE)
        masks = [i == h for i in hi]
        for c in range(3):
            row = jnp.broadcast_to(table[c * HP + r : c * HP + r + 1, cols], (8, LANE))
            for k in range(len(idxs)):
                got = jnp.take_along_axis(row, lo[k], axis=1, mode="promise_in_bounds")
                out[k][c] = jnp.where(masks[k], got, out[k][c])
    return out


def scatter(idx_ref, parts_ref, acc_ref, count):
    acc_ref[...] = jnp.zeros(acc_ref.shape, jnp.float32)
    lo_iota = lax.broadcasted_iota(jnp.int32, (LO, LANE), 0)
    hi_iota = lax.broadcasted_iota(jnp.int32, (HP, LANE), 0)

    def step(i, carry):
        hot, moved = [], []
        for t in range(RC):
            row = i * RC + t
            ix = idx_ref[pl.ds(row, 1), :]
            hot.append(jnp.where(lo_iota == (ix & (LO - 1)), 1.0, 0.0).astype(jnp.bfloat16))
            mask = hi_iota == (ix >> 8)
            moved.append(
                jnp.concatenate(
                    [
                        jnp.where(mask, parts_ref[pl.ds(p * count + row, 1), :], 0.0).astype(jnp.bfloat16)
                        for p in range(9)
                    ],
                    axis=0,
                )
            )
        acc_ref[...] += lax.dot_general(
            jnp.concatenate(hot, axis=1),
            jnp.concatenate(moved, axis=1),
            (((1,), (1,)), ((), ())),
            preferred_element_type=jnp.float32,
        )
        return carry

    lax.fori_loop(0, count // RC, step, 0)
    total = jnp.transpose(acc_ref[...])
    n = 3 * HP
    return total[:n] + total[n : 2 * n] + total[2 * n :]


def rhs_kernel(col_ref, map_ref, fine_ref, out_ref, idx_ref, parts_ref, acc_ref, *, own):
    count = map_ref.shape[0]
    idx_ref[...] = map_ref[...] - col_ref[0] * own
    for c in range(3):
        pieces = split3(0.5 * fine_ref[c * count // 2 : (c + 1) * count // 2, :])
        for s in range(3):
            for k in range(2):
                at = (s * 3 + c) * count + k * count // 2
                parts_ref[at : at + count // 2, :] = pieces[s]
    out_ref[...] = scatter(idx_ref, parts_ref, acc_ref, count)


def apply_elements(col_ref, table, conn_ref, grads_ref, moduli_ref, idx_ref, parts_ref, energy_ref, rows, own):
    per = moduli_ref.shape[0] // 2
    idx_ref[...] = conn_ref[...] - col_ref[0] * own
    energy_ref[...] = jnp.zeros((8, LANE), jnp.float32)

    def step(j, carry):
        at = j * 8
        idxs = [idx_ref[pl.ds(k * per + at, 8), :] for k in range(4)]
        v = gather(table, idxs, rows)
        g = [[grads_ref[pl.ds((d * 3 + a) * per + at, 8), :] for d in range(3)] for a in range(3)]
        lam = moduli_ref[pl.ds(at, 8), :]
        mu = moduli_ref[pl.ds(per + at, 8), :]
        w = [[v[a][i] - v[3][i] for i in range(3)] for a in range(3)]
        grad = [[w[0][i] * g[0][j] + w[1][i] * g[1][j] + w[2][i] * g[2][j] for j in range(3)] for i in range(3)]
        strain = [[0.5 * (grad[i][j] + grad[j][i]) for j in range(3)] for i in range(3)]
        bulk = lam * (strain[0][0] + strain[1][1] + strain[2][2])
        stress = [[2.0 * mu * strain[i][j] + (bulk if i == j else 0.0) for j in range(3)] for i in range(3)]
        work = sum(stress[i][i] * strain[i][i] for i in range(3))
        work = work + 2.0 * (
            stress[0][1] * strain[0][1] + stress[0][2] * strain[0][2] + stress[1][2] * strain[1][2]
        )
        energy_ref[...] += work
        if parts_ref is not None:
            count = 4 * per
            for i in range(3):
                f = [sum(stress[i][j] * g[a][j] for j in range(3)) for a in range(3)]
                f.append(-(f[0] + f[1] + f[2]))
                for a in range(4):
                    pieces = split3(f[a])
                    for s in range(3):
                        parts_ref[pl.ds((s * 3 + i) * count + a * per + at, 8), :] = pieces[s]
        return carry

    lax.fori_loop(0, per // 8, step, 0)
    return jnp.sum(energy_ref[...])


def own_rows(own):
    r = lax.broadcasted_iota(jnp.int32, (3 * HP, LO), 0) & (HP - 1)
    return r < own // LO


def per_component(x):
    return jnp.concatenate([x, x, x], axis=0)


def add_halo(own_part, col, recv_ref, own, rows):
    size = recv_ref.shape[0]
    k = CI // LO
    before = jnp.maximum(col - 1, 0)
    after = jnp.minimum(col + 1, size - 1)
    down = recv_ref[pl.ds(before, 1)][0]
    up = recv_ref[pl.ds(after, 1)][0]
    down = jnp.where(col > 0, down, 0.0)
    up = jnp.where(col < size - 1, up, 0.0)
    blank = [jnp.zeros((HP - k, LO), jnp.float32), jnp.zeros((own // LO, LO), jnp.float32)]
    pieces = []
    for c in range(3):
        pieces.append(down[c * k : (c + 1) * k])
        pieces.append(jnp.zeros((own // LO - k, LO), jnp.float32))
        pieces.append(up[c * k : (c + 1) * k])
        pieces.append(jnp.zeros((HP - own // LO - k, LO), jnp.float32))
    del blank
    return own_part + jnp.concatenate(pieces, axis=0)


def pack(msg_ref, table, col, scalars, own):
    size = msg_ref.shape[0]
    k = CI // LO
    base = own // LO
    lower = [table[c * HP : c * HP + k] for c in range(3)]
    upper = [table[c * HP + base : c * HP + base + k] for c in range(3)]
    rid = lax.broadcasted_iota(jnp.int32, (HP - 3 * k, LO), 0)
    tail = jnp.zeros((HP - 3 * k, LO), jnp.float32)
    for i, s in enumerate(scalars):
        tail = jnp.where(rid == i, s, tail)
    msg_ref[...] = jnp.broadcast_to(
        jnp.concatenate([jnp.zeros((3 * k, LO), jnp.float32), tail], axis=0)[None], msg_ref.shape
    )

    @pl.when(col > 0)
    def _():
        msg_ref[pl.ds(col - 1, 1)] = jnp.concatenate(lower + [tail], axis=0)[None]

    @pl.when(col < size - 1)
    def _():
        msg_ref[pl.ds(col + 1, 1)] = jnp.concatenate(upper + [tail], axis=0)[None]


def reduced(recv_ref, i, width):
    k = 3 * CI // LO if width == HP else 0
    return jnp.sum(recv_ref[:, k + i : k + i + 1, 0:1])


def first_kernel(col_ref, sum_ref, halo_ref, mass_ref, conn_ref, grads_ref, moduli_ref,
                 msg_ref, r_ref, f_ref, idx_ref, parts_ref, acc_ref, energy_ref, *, own, rows):
    col = col_ref[0]
    r_ref[...] = add_halo(sum_ref[...], col, halo_ref, own, rows)
    mine = own_rows(own)
    r = jnp.where(mine, r_ref[...], 0.0)
    mass = per_component(mass_ref[...])
    rr = jnp.sum(r * r)
    energy = apply_elements(col_ref, r_ref, conn_ref, grads_ref, moduli_ref, idx_ref, parts_ref, energy_ref, rows, own)
    curv = energy + jnp.sum(mass * r * r)
    f = scatter(idx_ref, parts_ref, acc_ref, idx_ref.shape[0])
    f_ref[...] = f
    pack(msg_ref, f, col, [rr, curv], own)


def second_kernel(col_ref, recv_ref, r0_ref, f0_ref, mass_ref, conn_ref, grads_ref, moduli_ref,
                  msg_ref, r_ref, f_ref, image_ref, sc_ref, idx_ref, parts_ref, acc_ref, energy_ref, *, own, rows):
    col = col_ref[0]
    mass = per_component(mass_ref[...])
    rr0 = reduced(recv_ref, 0, HP)
    curv0 = reduced(recv_ref, 1, HP)
    alpha0 = rr0 / curv0
    image = add_halo(f0_ref[...] + mass * r0_ref[...], col, recv_ref, own, rows)
    image_ref[...] = image
    r_ref[...] = r0_ref[...] - alpha0 * image
    r = jnp.where(own_rows(own), r_ref[...], 0.0)
    rr = jnp.sum(r * r)
    cross = jnp.sum(r * image)
    energy = apply_elements(col_ref, r_ref, conn_ref, grads_ref, moduli_ref, idx_ref, parts_ref, energy_ref, rows, own)
    own_curv = energy + jnp.sum(mass * r * r)
    f = scatter(idx_ref, parts_ref, acc_ref, idx_ref.shape[0])
    f_ref[...] = f
    pack(msg_ref, f, col, [rr, own_curv, cross], own)
    sc_ref[0] = rr0
    sc_ref[1] = curv0
    sc_ref[2] = alpha0


def third_kernel(col_ref, sc_ref, recv_ref, r0_ref, r1_ref, f1_ref, image_ref, mass_ref, conn_ref, grads_ref,
                 moduli_ref, msg_ref, r_ref, d_ref, x_ref, out_sc_ref, idx_ref, energy_ref, *, own, rows):
    col = col_ref[0]
    mass = per_component(mass_ref[...])
    rr0, curv0, alpha0 = sc_ref[0], sc_ref[1], sc_ref[2]
    rr1 = reduced(recv_ref, 0, HP)
    own_curv = reduced(recv_ref, 1, HP)
    cross = reduced(recv_ref, 2, HP)
    beta = rr1 / rr0
    curv1 = own_curv + 2.0 * beta * cross + beta * beta * curv0
    alpha1 = rr1 / curv1
    r1 = r1_ref[...]
    image = add_halo(f1_ref[...] + mass * r1, col, recv_ref, own, rows) + beta * image_ref[...]
    d = r1 + beta * r0_ref[...]
    d_ref[...] = d
    x_ref[...] = alpha0 * r0_ref[...] + alpha1 * d
    r_ref[...] = r1 - alpha1 * image
    r = jnp.where(own_rows(own), r_ref[...], 0.0)
    rr = jnp.sum(r * r)
    cross = jnp.sum(r * image)
    energy = apply_elements(col_ref, r_ref, conn_ref, grads_ref, moduli_ref, idx_ref, None, energy_ref, rows, own)
    own_curv = energy + jnp.sum(mass * r * r)
    rid = lax.broadcasted_iota(jnp.int32, msg_ref.shape, 1)
    msg_ref[...] = jnp.where(rid == 0, rr, jnp.where(rid == 1, own_curv, cross))
    out_sc_ref[0] = rr1
    out_sc_ref[1] = curv1


def last_kernel(col_ref, sc_ref, recv_ref, r_ref, d_ref, x_ref, map_ref, out_ref, table_ref, *, own, rows):
    col = col_ref[0]
    rr1, curv1 = sc_ref[0], sc_ref[1]
    rr2 = reduced(recv_ref, 0, 8)
    own_curv = reduced(recv_ref, 1, 8)
    cross = reduced(recv_ref, 2, 8)
    beta = rr2 / rr1
    curv2 = own_curv + 2.0 * beta * cross + beta * beta * curv1
    alpha2 = rr2 / curv2
    table_ref[...] = 0.5 * (x_ref[...] + alpha2 * (r_ref[...] + beta * d_ref[...]))
    per = map_ref.shape[0] // 2

    def step(j, carry):
        at = j * 8
        idxs = [map_ref[pl.ds(k * per + at, 8), :] - col * own for k in range(2)]
        v = gather(table_ref, idxs, rows)
        for c in range(3):
            out_ref[pl.ds(c * per + at, 8), :] = v[0][c] + v[1][c]
        return carry

    lax.fori_loop(0, per // 8, step, 0)


def call(kernel, outs, scratch, smem_in, n_in):
    vm = pl.BlockSpec(memory_space=pltpu.VMEM)
    sm = pl.BlockSpec(memory_space=pltpu.SMEM)
    out_specs = [sm if len(o.shape) == 1 else vm for o in outs]
    return pl.pallas_call(
        kernel,
        out_shape=outs,
        in_specs=[sm] * smem_in + [vm] * n_in,
        out_specs=out_specs,
        scratch_shapes=scratch,
    )


def body(fine_res, node_map, connect, grads, moduli, mass):
    size = lax.axis_size("sub")
    groups = lax.axis_size("grp")
    own = mass.shape[0]
    fine = node_map.shape[1]
    elems = connect.shape[1]
    rows = (own + CI) // LO
    col = lax.axis_index("sub").astype(jnp.int32).reshape(1)
    f32 = functools.partial(jax.ShapeDtypeStruct, dtype=jnp.float32)
    table = f32((3 * HP, LO))
    msg = f32((size, HP, LO))
    map2 = node_map.reshape(2 * fine // LANE, LANE)
    fine2 = fine_res.reshape(3 * fine // LANE, LANE)
    conn2 = connect.reshape(4 * elems // LANE, LANE)
    grads2 = grads.reshape(9 * elems // LANE, LANE)
    moduli2 = moduli.reshape(2 * elems // LANE, LANE)
    acc = pltpu.VMEM((LO, 9 * HP), jnp.float32)
    fcount = 2 * fine // LANE
    ecount = 4 * elems // LANE

    (partial,) = call(
        functools.partial(rhs_kernel, own=own),
        [table],
        [pltpu.VMEM((fcount, LANE), jnp.int32), pltpu.VMEM((9 * fcount, LANE), jnp.float32), acc],
        1,
        2,
    )(col, map2, fine2)
    summed = partial
    for k in range(1, groups):
        summed = summed + lax.ppermute(partial, "grp", [(i, (i + k) % groups) for i in range(groups)])
    k = CI // LO
    s3 = summed.reshape(3, HP, LO)
    lower = s3[:, :k].reshape(3 * k, LO)
    upper = s3[:, own // LO : own // LO + k].reshape(3 * k, LO)
    mass2 = mass.reshape(own // LO, LO)
    down = jnp.concatenate([lower, mass2[:k]], axis=0)
    up = jnp.concatenate([upper, jnp.zeros((k, LO), jnp.float32)], axis=0)
    c0 = col[0]
    halo = jnp.zeros((size, HP, LO), jnp.float32)
    halo = jnp.where((jnp.arange(size) == c0 - 1)[:, None, None], down[None], halo)
    halo = jnp.where((jnp.arange(size) == c0 + 1)[:, None, None], up[None], halo)
    halo = lax.all_to_all(halo, "sub", 0, 0)
    mass_next = lax.dynamic_slice_in_dim(halo, jnp.minimum(c0 + 1, size - 1), 1, 0)[0, 3 * k :]
    mass_ext = jnp.concatenate([mass2, mass_next, jnp.zeros((HP - own // LO - k, LO), jnp.float32)], axis=0)

    idx = pltpu.VMEM((ecount, LANE), jnp.int32)
    parts = pltpu.VMEM((9 * ecount, LANE), jnp.float32)
    energy = pltpu.VMEM((8, LANE), jnp.float32)
    kw = dict(own=own, rows=rows)
    m0, r0, f0 = call(functools.partial(first_kernel, **kw), [msg, table, table], [idx, parts, acc, energy], 1, 6)(
        col, summed, halo, mass_ext, conn2, grads2, moduli2
    )
    m0 = lax.all_to_all(m0, "sub", 0, 0)
    m1, r1, f1, image, sc = call(
        functools.partial(second_kernel, **kw), [msg, table, table, table, f32((3,))], [idx, parts, acc, energy], 1, 7
    )(col, m0, r0, f0, mass_ext, conn2, grads2, moduli2)
    m1 = lax.all_to_all(m1, "sub", 0, 0)
    m2, r2, d1, x2, sc = call(
        functools.partial(third_kernel, **kw), [f32((size, 8, LANE)), table, table, table, f32((2,))], [idx, energy], 2, 9
    )(col, sc, m1, r0, r1, f1, image, mass_ext, conn2, grads2, moduli2)
    m2 = lax.all_to_all(m2, "sub", 0, 0)
    (out,) = call(
        functools.partial(last_kernel, **kw), [f32((3 * fine // LANE, LANE))], [pltpu.VMEM((3 * HP, LO), jnp.float32)], 2, 5
    )(col, sc, m2, r2, d1, x2, map2)
    return out.reshape(3, fine)


def solution(mesh):
    in_specs = (
        P(None, ("grp", "sub")),
        P(None, ("grp", "sub")),
        P(None, "sub"),
        P(None, None, "sub"),
        P(None, "sub"),
        P("sub"),
    )
    out_specs = P(None, ("grp", "sub"))
    return jax.shard_map(body, mesh=mesh, in_specs=in_specs, out_specs=out_specs, check_vma=False)
```

```python
import functools

import jax
import jax.numpy as jnp
from jax import lax
from jax.experimental import pallas as pl
from jax.experimental.pallas import tpu as pltpu
from jax.sharding import PartitionSpec as P

CI = 1024
LANE = 128
LO = 256
HP = 16
RC = 32


def split3(x):
    a = x.astype(jnp.bfloat16).astype(jnp.float32)
    r = x - a
    b = r.astype(jnp.bfloat16).astype(jnp.float32)
    return a, b, r - b


def gather(table, idxs, rows):
    out = []
    for ix in idxs:
        lo = ix & (LANE - 1)
        hi = ix >> 7
        got = [jnp.zeros((8, LANE), jnp.float32)] * 3
        for h in range(rows * LO // LANE):
            r, half = divmod(h, LO // LANE)
            mask = hi == h
            for c in range(3):
                row = table[c * HP + r : c * HP + r + 1, half * LANE : (half + 1) * LANE]
                row = jnp.broadcast_to(row, (8, LANE))
                moved = jnp.take_along_axis(row, lo, axis=1, mode="promise_in_bounds")
                got[c] = jnp.where(mask, moved, got[c])
        out.append(got)
    return out


def scatter(idx_ref, parts_ref, acc_ref, count):
    acc_ref[...] = jnp.zeros(acc_ref.shape, jnp.float32)
    lo_iota = lax.broadcasted_iota(jnp.int32, (LO, LANE), 0)
    hi_iota = lax.broadcasted_iota(jnp.int32, (HP, LANE), 0)

    def step(i, carry):
        hot, moved = [], []
        for t in range(RC):
            row = i * RC + t
            ix = idx_ref[pl.ds(row, 1), :]
            hot.append(jnp.where(lo_iota == (ix & (LO - 1)), 1.0, 0.0).astype(jnp.bfloat16))
            mask = hi_iota == (ix >> 8)
            moved.append(
                jnp.concatenate(
                    [
                        jnp.where(mask, parts_ref[pl.ds(p * count + row, 1), :], 0.0).astype(jnp.bfloat16)
                        for p in range(9)
                    ],
                    axis=0,
                )
            )
        acc_ref[...] += lax.dot_general(
            jnp.concatenate(hot, axis=1),
            jnp.concatenate(moved, axis=1),
            (((1,), (1,)), ((), ())),
            preferred_element_type=jnp.float32,
        )
        return carry

    lax.fori_loop(0, count // RC, step, 0)
    total = jnp.transpose(acc_ref[...])
    n = 3 * HP
    return total[:n] + total[n : 2 * n] + total[2 * n :]


def lines(ref, lead, dst, base, f=lambda x: x):
    n = ref.shape[-1] // LANE
    for q in range(n):
        dst[base + q : base + q + 1, :] = f(ref[lead + (slice(q * LANE, (q + 1) * LANE),)])


def rhs_kernel(col_ref, map_ref, fine_ref, mass_ref, out_ref, lower_ref, upper_ref, idx_ref,
               half_ref, parts_ref, acc_ref, *, own):
    half = map_ref.shape[1] // LANE
    count = 2 * half
    shift = col_ref[0] * own
    for k in range(2):
        lines(map_ref, (slice(k, k + 1),), idx_ref, k * half, lambda x: x - shift)
    for c in range(3):
        lines(fine_ref, (slice(c, c + 1),), half_ref, c * half)
    for c in range(3):
        pieces = split3(0.5 * half_ref[c * half : (c + 1) * half, :])
        for s in range(3):
            for k in range(2):
                at = (s * 3 + c) * count + k * half
                parts_ref[at : at + half, :] = pieces[s]
    table = scatter(idx_ref, parts_ref, acc_ref, count)
    out_ref[...] = table
    k = CI // LO
    lower, upper = shared(table, own)
    mass = jnp.concatenate([mass_ref[pl.ds(0, k, stride=2), :], mass_ref[pl.ds(1, k, stride=2), :]], axis=1)
    lower_ref[...] = jnp.concatenate([lower, mass], axis=0)
    upper_ref[...] = upper


def prep_kernel(col_ref, conn_ref, grads_ref, moduli_ref, idx_ref, g_ref, m_ref, *, own):
    per = moduli_ref.shape[1] // LANE
    shift = col_ref[0] * own
    for a in range(4):
        lines(conn_ref, (slice(a, a + 1),), idx_ref, a * per, lambda x: x - shift)
    for d in range(3):
        for a in range(3):
            lines(grads_ref, (d, slice(a, a + 1)), g_ref, (d * 3 + a) * per)
    for i in range(2):
        lines(moduli_ref, (slice(i, i + 1),), m_ref, i * per)


def shared(table, own):
    k = CI // LO
    base = own // LO
    lower = jnp.concatenate([table[c * HP : c * HP + k] for c in range(3)], axis=0)
    upper = jnp.concatenate([table[c * HP + base : c * HP + base + k] for c in range(3)], axis=0)
    return lower, upper


def halo_kernel(col_ref, table_ref, before_ref, after_ref, mass_ref, out_ref, mass_out_ref, *, own, size):
    col = col_ref[0]
    k = CI // LO
    after = after_ref[...]
    out_ref[...] = add_halo(table_ref[...], col, before_ref[...], after[: 3 * k], own, size)
    mine = jnp.concatenate(
        [mass_ref[pl.ds(0, own // LO, stride=2), :], mass_ref[pl.ds(1, own // LO, stride=2), :]], axis=1
    )
    pad = jnp.zeros((HP - own // LO - k, LO), jnp.float32)
    mass_out_ref[...] = jnp.concatenate([mine, after[3 * k :], pad], axis=0)


def apply_elements(table, idx_ref, grads_ref, moduli_ref, parts_ref, energy_ref, rows):
    per = moduli_ref.shape[0] // 2
    energy_ref[...] = jnp.zeros((8, LANE), jnp.float32)

    def step(j, carry):
        at = j * 8
        idxs = [idx_ref[pl.ds(k * per + at, 8), :] for k in range(4)]
        v = gather(table, idxs, rows)
        g = [[grads_ref[pl.ds((d * 3 + a) * per + at, 8), :] for d in range(3)] for a in range(3)]
        lam = moduli_ref[pl.ds(at, 8), :]
        mu = moduli_ref[pl.ds(per + at, 8), :]
        w = [[v[a][i] - v[3][i] for i in range(3)] for a in range(3)]
        grad = [[w[0][i] * g[0][j] + w[1][i] * g[1][j] + w[2][i] * g[2][j] for j in range(3)] for i in range(3)]
        strain = [[0.5 * (grad[i][j] + grad[j][i]) for j in range(3)] for i in range(3)]
        bulk = lam * (strain[0][0] + strain[1][1] + strain[2][2])
        stress = [[2.0 * mu * strain[i][j] + (bulk if i == j else 0.0) for j in range(3)] for i in range(3)]
        work = sum(stress[i][i] * strain[i][i] for i in range(3))
        work = work + 2.0 * (
            stress[0][1] * strain[0][1] + stress[0][2] * strain[0][2] + stress[1][2] * strain[1][2]
        )
        energy_ref[...] += work
        if parts_ref is not None:
            count = 4 * per
            for i in range(3):
                f = [sum(stress[i][j] * g[a][j] for j in range(3)) for a in range(3)]
                f.append(-(f[0] + f[1] + f[2]))
                for a in range(4):
                    pieces = split3(f[a])
                    for s in range(3):
                        parts_ref[pl.ds((s * 3 + i) * count + a * per + at, 8), :] = pieces[s]
        return carry

    lax.fori_loop(0, per // 8, step, 0)
    return jnp.sum(energy_ref[...])


def own_rows(own):
    r = lax.broadcasted_iota(jnp.int32, (3 * HP, LO), 0) & (HP - 1)
    return r < own // LO


def per_component(x):
    return jnp.concatenate([x, x, x], axis=0)


def add_halo(own_part, col, down, up, own, size):
    k = CI // LO
    down = jnp.where(col > 0, down, 0.0)
    up = jnp.where(col < size - 1, up, 0.0)
    pieces = []
    for c in range(3):
        pieces.append(down[c * k : (c + 1) * k])
        pieces.append(jnp.zeros((own // LO - k, LO), jnp.float32))
        pieces.append(up[c * k : (c + 1) * k])
        pieces.append(jnp.zeros((HP - own // LO - k, LO), jnp.float32))
    return own_part + jnp.concatenate(pieces, axis=0)


def add_received(own_part, col, recv_ref, own):
    size = recv_ref.shape[0]
    k = 3 * CI // LO
    down = recv_ref[pl.ds(jnp.maximum(col - 1, 0), 1)][0]
    up = recv_ref[pl.ds(jnp.minimum(col + 1, size - 1), 1)][0]
    return add_halo(own_part, col, down[:k], up[:k], own, size)


def pack(msg_ref, table, col, scalars, own):
    size = msg_ref.shape[0]
    k = CI // LO
    lower, upper = shared(table, own)
    rid = lax.broadcasted_iota(jnp.int32, (HP - 3 * k, LO), 0)
    tail = jnp.zeros((HP - 3 * k, LO), jnp.float32)
    for i, s in enumerate(scalars):
        tail = jnp.where(rid == i, s, tail)
    msg_ref[...] = jnp.broadcast_to(
        jnp.concatenate([jnp.zeros((3 * k, LO), jnp.float32), tail], axis=0)[None], msg_ref.shape
    )

    @pl.when(col > 0)
    def _():
        msg_ref[pl.ds(col - 1, 1)] = jnp.concatenate([lower, tail], axis=0)[None]

    @pl.when(col < size - 1)
    def _():
        msg_ref[pl.ds(col + 1, 1)] = jnp.concatenate([upper, tail], axis=0)[None]


def reduced(recv_ref, i, width):
    k = 3 * CI // LO if width == HP else 0
    return jnp.sum(recv_ref[:, k + i : k + i + 1, 0:1])


def first_kernel(col_ref, *refs, own, rows, groups):
    sum_refs = refs[:groups]
    mass_ref, idx_ref, grads_ref, moduli_ref, msg_ref, r_ref, f_ref, parts_ref, acc_ref, energy_ref = refs[groups:]
    total = sum_refs[0][...]
    for ref in sum_refs[1:]:
        total = total + ref[...]
    r_ref[...] = total
    r = jnp.where(own_rows(own), total, 0.0)
    mass = per_component(mass_ref[...])
    rr = jnp.sum(r * r)
    energy = apply_elements(r_ref, idx_ref, grads_ref, moduli_ref, parts_ref, energy_ref, rows)
    curv = energy + jnp.sum(mass * r * r)
    f = scatter(idx_ref, parts_ref, acc_ref, idx_ref.shape[0])
    f_ref[...] = f
    pack(msg_ref, f, col_ref[0], [rr, curv], own)


def second_kernel(col_ref, recv_ref, r0_ref, f0_ref, mass_ref, idx_ref, grads_ref, moduli_ref,
                  msg_ref, r_ref, f_ref, image_ref, sc_ref, parts_ref, acc_ref, energy_ref, *, own, rows):
    col = col_ref[0]
    mass = per_component(mass_ref[...])
    rr0 = reduced(recv_ref, 0, HP)
    curv0 = reduced(recv_ref, 1, HP)
    alpha0 = rr0 / curv0
    image = add_received(f0_ref[...] + mass * r0_ref[...], col, recv_ref, own)
    image_ref[...] = image
    r_ref[...] = r0_ref[...] - alpha0 * image
    r = jnp.where(own_rows(own), r_ref[...], 0.0)
    rr = jnp.sum(r * r)
    cross = jnp.sum(r * image)
    energy = apply_elements(r_ref, idx_ref, grads_ref, moduli_ref, parts_ref, energy_ref, rows)
    own_curv = energy + jnp.sum(mass * r * r)
    f = scatter(idx_ref, parts_ref, acc_ref, idx_ref.shape[0])
    f_ref[...] = f
    pack(msg_ref, f, col, [rr, own_curv, cross], own)
    sc_ref[0] = rr0
    sc_ref[1] = curv0
    sc_ref[2] = alpha0


def third_kernel(col_ref, sc_ref, recv_ref, r0_ref, r1_ref, f1_ref, image_ref, mass_ref, idx_ref, grads_ref,
                 moduli_ref, msg_ref, r_ref, d_ref, x_ref, out_sc_ref, energy_ref, *, own, rows):
    col = col_ref[0]
    mass = per_component(mass_ref[...])
    rr0, curv0, alpha0 = sc_ref[0], sc_ref[1], sc_ref[2]
    rr1 = reduced(recv_ref, 0, HP)
    own_curv = reduced(recv_ref, 1, HP)
    cross = reduced(recv_ref, 2, HP)
    beta = rr1 / rr0
    curv1 = own_curv + 2.0 * beta * cross + beta * beta * curv0
    alpha1 = rr1 / curv1
    r1 = r1_ref[...]
    image = add_received(f1_ref[...] + mass * r1, col, recv_ref, own) + beta * image_ref[...]
    d = r1 + beta * r0_ref[...]
    d_ref[...] = d
    x_ref[...] = alpha0 * r0_ref[...] + alpha1 * d
    r_ref[...] = r1 - alpha1 * image
    r = jnp.where(own_rows(own), r_ref[...], 0.0)
    rr = jnp.sum(r * r)
    cross = jnp.sum(r * image)
    energy = apply_elements(r_ref, idx_ref, grads_ref, moduli_ref, None, energy_ref, rows)
    own_curv = energy + jnp.sum(mass * r * r)
    rid = lax.broadcasted_iota(jnp.int32, msg_ref.shape, 1)
    msg_ref[...] = jnp.where(rid == 0, rr, jnp.where(rid == 1, own_curv, cross))
    out_sc_ref[0] = rr1
    out_sc_ref[1] = curv1


def last_kernel(sc_ref, recv_ref, r_ref, d_ref, x_ref, idx_ref, out_ref, table_ref, *, rows):
    rr1, curv1 = sc_ref[0], sc_ref[1]
    rr2 = reduced(recv_ref, 0, 8)
    own_curv = reduced(recv_ref, 1, 8)
    cross = reduced(recv_ref, 2, 8)
    beta = rr2 / rr1
    curv2 = own_curv + 2.0 * beta * cross + beta * beta * curv1
    alpha2 = rr2 / curv2
    table_ref[...] = 0.5 * (x_ref[...] + alpha2 * (r_ref[...] + beta * d_ref[...]))
    per = idx_ref.shape[0] // 2
    for j in range(per // 8):
        v = gather(table_ref, [idx_ref[k * per + j * 8 : k * per + j * 8 + 8, :] for k in range(2)], rows)
        for c in range(3):
            got = v[0][c] + v[1][c]
            for q in range(8):
                at = (j * 8 + q) * LANE
                out_ref[c : c + 1, at : at + LANE] = got[q : q + 1, :]


def call(kernel, args, outs, scratch=()):
    spaces = {"s": pltpu.SMEM, "v": pltpu.VMEM, "h": pltpu.VMEM}
    arrays = [pltpu.with_memory_space_constraint(x, pltpu.VMEM) if m == "v" else x for x, m in args]
    return pl.pallas_call(
        kernel,
        out_shape=[o for o, _ in outs],
        in_specs=[pl.BlockSpec(memory_space=spaces[m]) for _, m in args],
        out_specs=[pl.BlockSpec(memory_space=spaces[m]) for _, m in outs],
        scratch_shapes=list(scratch),
    )(*arrays)


def rotated(x, axis, by):
    n = lax.axis_size(axis)
    return lax.ppermute(x, axis, [(i, (i + by) % n) for i in range(n)])


def body(fine_res, node_map, connect, grads, moduli, mass):
    size = lax.axis_size("sub")
    groups = lax.axis_size("grp")
    own = mass.shape[0]
    fine = node_map.shape[1]
    elems = connect.shape[1]
    rows = (own + CI) // LO
    k = CI // LO
    col = lax.axis_index("sub").astype(jnp.int32).reshape(1)
    fcount = 2 * fine // LANE
    ecount = 4 * elems // LANE

    def kept(*shape, dtype=jnp.float32):
        return pltpu.VMEM(shape, dtype), "v"

    table = kept(3 * HP, LO)
    msg = kept(size, HP, LO)
    scalars = lambda n: (jax.ShapeDtypeStruct((n,), jnp.float32), "s")
    acc = pltpu.VMEM((LO, 9 * HP), jnp.float32)
    parts = pltpu.VMEM((9 * ecount, LANE), jnp.float32)
    energy = pltpu.VMEM((8, LANE), jnp.float32)
    mass2 = mass.reshape(own // LANE, LANE)

    partial, lower, upper, map_idx = call(
        functools.partial(rhs_kernel, own=own),
        [(col, "s"), (node_map, "h"), (fine_res, "h"), (mass2, "h")],
        [table, kept(4 * k, LO), kept(3 * k, LO), kept(fcount, LANE, dtype=jnp.int32)],
        [pltpu.VMEM((3 * fcount // 2, LANE), jnp.float32), pltpu.VMEM((9 * fcount, LANE), jnp.float32), acc],
    )
    before = rotated(upper, "sub", 1)
    after = rotated(lower, "sub", -1)
    idx, g, mod = call(
        functools.partial(prep_kernel, own=own),
        [(col, "s"), (connect, "h"), (grads, "h"), (moduli, "h")],
        [kept(ecount, LANE, dtype=jnp.int32), kept(9 * elems // LANE, LANE), kept(2 * elems // LANE, LANE)],
    )
    part, mass_ext = call(
        functools.partial(halo_kernel, own=own, size=size),
        [(col, "s"), (partial, "v"), (before, "v"), (after, "v"), (mass2, "h")],
        [table, kept(HP, LO)],
    )
    sums = [part] + [rotated(part, "grp", i) for i in range(1, groups)]
    elements = [(mass_ext, "v"), (idx, "v"), (g, "v"), (mod, "v")]
    kw = dict(own=own, rows=rows)
    m0, r0, f0 = call(
        functools.partial(first_kernel, groups=groups, **kw),
        [(col, "s")] + [(x, "v") for x in sums] + elements,
        [msg, table, table],
        [parts, acc, energy],
    )
    m0 = lax.all_to_all(m0, "sub", 0, 0)
    m1, r1, f1, image, sc = call(
        functools.partial(second_kernel, **kw),
        [(col, "s"), (m0, "v"), (r0, "v"), (f0, "v")] + elements,
        [msg, table, table, table, scalars(3)],
        [parts, acc, energy],
    )
    m1 = lax.all_to_all(m1, "sub", 0, 0)
    m2, r2, d1, x2, sc = call(
        functools.partial(third_kernel, **kw),
        [(col, "s"), (sc, "s"), (m1, "v"), (r0, "v"), (r1, "v"), (f1, "v"), (image, "v")] + elements,
        [kept(size, 8, LANE), table, table, table, scalars(2)],
        [energy],
    )
    m2 = lax.all_to_all(m2, "sub", 0, 0)
    (out,) = call(
        functools.partial(last_kernel, rows=rows),
        [(sc, "s"), (m2, "v"), (r2, "v"), (d1, "v"), (x2, "v"), (map_idx, "v")],
        [(jax.ShapeDtypeStruct((3, fine), jnp.float32), "h")],
        [pltpu.VMEM((3 * HP, LO), jnp.float32)],
    )
    return out


def solution(mesh):
    in_specs = (
        P(None, ("grp", "sub")),
        P(None, ("grp", "sub")),
        P(None, "sub"),
        P(None, None, "sub"),
        P(None, "sub"),
        P("sub"),
    )
    out_specs = P(None, ("grp", "sub"))
    return jax.shard_map(body, mesh=mesh, in_specs=in_specs, out_specs=out_specs, check_vma=False)
```

```python
import functools

import jax
import jax.numpy as jnp
from jax import lax
from jax.experimental import pallas as pl
from jax.experimental.pallas import tpu as pltpu
from jax.sharding import PartitionSpec as P

CI = 1024
LANE = 128
LO = 256
HP = 16
RC = 32

PAIRS = ((0, 0), (1, 1), (2, 2), (0, 1), (0, 2), (1, 2))
SYM = ((0, 3, 4), (3, 1, 5), (4, 5, 2))


def split3(x):
    a = x.astype(jnp.bfloat16).astype(jnp.float32)
    r = x - a
    b = r.astype(jnp.bfloat16).astype(jnp.float32)
    return a, b, r - b


def gather(table, idxs, rows):
    out = []
    for ix in idxs:
        lo = ix & (LANE - 1)
        hi = ix >> 7
        got = [jnp.zeros((8, LANE), jnp.float32)] * 3
        for h in range(rows * LO // LANE):
            r, half = divmod(h, LO // LANE)
            mask = hi == h
            for c in range(3):
                row = table[c * HP + r : c * HP + r + 1, half * LANE : (half + 1) * LANE]
                row = jnp.broadcast_to(row, (8, LANE))
                moved = jnp.take_along_axis(row, lo, axis=1, mode="promise_in_bounds")
                got[c] = jnp.where(mask, moved, got[c])
        out.append(got)
    return out


def scatter(idx_ref, parts_ref, acc_ref, count):
    acc_ref[...] = jnp.zeros(acc_ref.shape, jnp.float32)
    lo_iota = lax.broadcasted_iota(jnp.int32, (LO, LANE), 0)
    hi_iota = lax.broadcasted_iota(jnp.int32, (HP, LANE), 0)

    def step(i, carry):
        hot, moved = [], []
        for t in range(RC):
            row = i * RC + t
            ix = idx_ref[pl.ds(row, 1), :]
            hot.append(jnp.where(lo_iota == (ix & (LO - 1)), 1.0, 0.0).astype(jnp.bfloat16))
            mask = hi_iota == (ix >> 8)
            moved.append(
                jnp.concatenate(
                    [
                        jnp.where(mask, parts_ref[pl.ds(p * count + row, 1), :], 0.0).astype(jnp.bfloat16)
                        for p in range(9)
                    ],
                    axis=0,
                )
            )
        acc_ref[...] += lax.dot_general(
            jnp.concatenate(hot, axis=1),
            jnp.concatenate(moved, axis=1),
            (((1,), (1,)), ((), ())),
            preferred_element_type=jnp.float32,
        )
        return carry

    lax.fori_loop(0, count // RC, step, 0)
    total = jnp.transpose(acc_ref[...])
    n = 3 * HP
    return total[:n] + total[n : 2 * n] + total[2 * n :]


def lines(ref, lead, dst, base, f=lambda x: x):
    n = ref.shape[-1] // LANE
    for q in range(n):
        dst[base + q : base + q + 1, :] = f(ref[lead + (slice(q * LANE, (q + 1) * LANE),)])


def rhs_kernel(col_ref, map_ref, fine_ref, mass_ref, out_ref, lower_ref, upper_ref, idx_ref,
               half_ref, parts_ref, acc_ref, *, own):
    half = map_ref.shape[1] // LANE
    count = 2 * half
    shift = col_ref[0] * own
    for k in range(2):
        lines(map_ref, (slice(k, k + 1),), idx_ref, k * half, lambda x: x - shift)
    for c in range(3):
        lines(fine_ref, (slice(c, c + 1),), half_ref, c * half)
    for c in range(3):
        pieces = split3(0.5 * half_ref[c * half : (c + 1) * half, :])
        for s in range(3):
            for k in range(2):
                at = (s * 3 + c) * count + k * half
                parts_ref[at : at + half, :] = pieces[s]
    table = scatter(idx_ref, parts_ref, acc_ref, count)
    out_ref[...] = table
    k = CI // LO
    lower, upper = shared(table, own)
    mass = jnp.concatenate([mass_ref[pl.ds(0, k, stride=2), :], mass_ref[pl.ds(1, k, stride=2), :]], axis=1)
    lower_ref[...] = jnp.concatenate([lower, mass], axis=0)
    upper_ref[...] = upper


def prep_kernel(col_ref, conn_ref, grads_ref, moduli_ref, idx_ref, g_ref, m_ref, *, own):
    per = moduli_ref.shape[1] // LANE
    shift = col_ref[0] * own
    for a in range(4):
        lines(conn_ref, (slice(a, a + 1),), idx_ref, a * per, lambda x: x - shift)
    for d in range(3):
        for a in range(3):
            lines(grads_ref, (d, slice(a, a + 1)), g_ref, (d * 3 + a) * per)
    for i in range(2):
        lines(moduli_ref, (slice(i, i + 1),), m_ref, i * per)


def shared(table, own):
    k = CI // LO
    base = own // LO
    lower = jnp.concatenate([table[c * HP : c * HP + k] for c in range(3)], axis=0)
    upper = jnp.concatenate([table[c * HP + base : c * HP + base + k] for c in range(3)], axis=0)
    return lower, upper


def halo_kernel(col_ref, table_ref, before_ref, after_ref, mass_ref, moduli_ref, out_ref, mass_out_ref, *, own, size):
    col = col_ref[0]
    k = CI // LO
    after = after_ref[...]
    out_ref[...] = add_halo(table_ref[...], col, before_ref[...], after[: 3 * k], own, size)
    mine = jnp.concatenate(
        [mass_ref[pl.ds(0, own // LO, stride=2), :], mass_ref[pl.ds(1, own // LO, stride=2), :]], axis=1
    )
    pad = jnp.zeros((HP - own // LO - k, LO), jnp.float32)
    mass_out_ref[...] = jnp.concatenate([mine, after[3 * k :], pad], axis=0)


def apply_elements(table, idx_ref, grads_ref, moduli_ref, strain_ref, parts_ref, rows):
    per = moduli_ref.shape[0] // 2
    count = 4 * per

    def step(j, carry):
        at = j * 8
        v = gather(table, [idx_ref[pl.ds(k * per + at, 8), :] for k in range(4)], rows)
        g = [[grads_ref[pl.ds((d * 3 + a) * per + at, 8), :] for d in range(3)] for a in range(3)]
        w = [[v[a][i] - v[3][i] for i in range(3)] for a in range(3)]
        grad = [[w[0][i] * g[0][j] + w[1][i] * g[1][j] + w[2][i] * g[2][j] for j in range(3)] for i in range(3)]
        strain = [0.5 * (grad[i][j] + grad[j][i]) for i, j in PAIRS]
        for p in range(6):
            strain_ref[pl.ds(p * per + at, 8), :] = strain[p]
        if parts_ref is not None:
            lam = moduli_ref[pl.ds(at, 8), :]
            mu = moduli_ref[pl.ds(per + at, 8), :]
            stress = stresses(strain, lam, mu)
            for i in range(3):
                f = [sum(stress[SYM[i][j]] * g[a][j] for j in range(3)) for a in range(3)]
                f.append(-(f[0] + f[1] + f[2]))
                for a in range(4):
                    pieces = split3(f[a])
                    for s in range(3):
                        parts_ref[pl.ds((s * 3 + i) * count + a * per + at, 8), :] = pieces[s]
        return carry

    lax.fori_loop(0, per // 8, step, 0)


def stresses(strain, lam, mu):
    bulk = lam * (strain[0] + strain[1] + strain[2])
    return [2.0 * mu * strain[p] + (bulk if p < 3 else 0.0) for p in range(6)]


def work(stress, strain):
    diag = stress[0] * strain[0] + stress[1] * strain[1] + stress[2] * strain[2]
    return diag + 2.0 * (stress[3] * strain[3] + stress[4] * strain[4] + stress[5] * strain[5])


def own_rows(own):
    r = lax.broadcasted_iota(jnp.int32, (3 * HP, LO), 0) & (HP - 1)
    return r < own // LO


def per_component(x):
    return jnp.concatenate([x, x, x], axis=0)


def add_halo(own_part, col, down, up, own, size):
    k = CI // LO
    down = jnp.where(col > 0, down, 0.0)
    up = jnp.where(col < size - 1, up, 0.0)
    pieces = []
    for c in range(3):
        pieces.append(down[c * k : (c + 1) * k])
        pieces.append(jnp.zeros((own // LO - k, LO), jnp.float32))
        pieces.append(up[c * k : (c + 1) * k])
        pieces.append(jnp.zeros((HP - own // LO - k, LO), jnp.float32))
    return own_part + jnp.concatenate(pieces, axis=0)


def first_kernel(*refs, own, rows, groups):
    sum_refs = refs[:groups]
    idx_ref, grads_ref, moduli_ref, v_ref, f_ref, lower_ref, upper_ref, strain_ref, parts_ref, acc_ref = refs[groups:]
    total = sum_refs[0][...]
    for ref in sum_refs[1:]:
        total = total + ref[...]
    v_ref[...] = total
    apply_elements(v_ref, idx_ref, grads_ref, moduli_ref, strain_ref, parts_ref, rows)
    f = scatter(idx_ref, parts_ref, acc_ref, idx_ref.shape[0])
    f_ref[...] = f
    lower_ref[...], upper_ref[...] = shared(f, own)


def second_kernel(col_ref, before_ref, after_ref, v0_ref, f0_ref, mass_ref, idx_ref, grads_ref, moduli_ref,
                  v_ref, f_ref, lower_ref, upper_ref, strain_ref, parts_ref, acc_ref, *, own, rows, size):
    mass = per_component(mass_ref[...])
    v_ref[...] = add_halo(
        f0_ref[...] + mass * v0_ref[...], col_ref[0], before_ref[...], after_ref[...], own, size
    )
    apply_elements(v_ref, idx_ref, grads_ref, moduli_ref, strain_ref, parts_ref, rows)
    f = scatter(idx_ref, parts_ref, acc_ref, idx_ref.shape[0])
    f_ref[...] = f
    lower_ref[...], upper_ref[...] = shared(f, own)


def total(x):
    return jnp.sum(x, axis=(0, 1), keepdims=True)


def ratio(a, b):
    return jnp.where(b > 0.0, a / jnp.where(b > 0.0, b, 1.0), 0.0)


def third_kernel(col_ref, before_ref, after_ref, v0_ref, v1_ref, f1_ref, s0_ref, s1_ref, mass_ref, idx_ref,
                 grads_ref, moduli_ref, msg_ref, v2_ref, s2_ref, *, own, rows, size):
    mass = per_component(mass_ref[...])
    v2 = add_halo(f1_ref[...] + mass * v1_ref[...], col_ref[0], before_ref[...], after_ref[...], own, size)
    v2_ref[...] = v2
    mine = own_rows(own)
    x0 = jnp.where(mine, v0_ref[...], 0.0)
    x1 = jnp.where(mine, v1_ref[...], 0.0)
    x2 = jnp.where(mine, v2, 0.0)
    rr0 = total(x0 * x0)
    n1 = total(x1 * x1)
    usable = (rr0 > 0.0) & (n1 > 0.0)
    s = jnp.where(usable, jnp.sqrt(jnp.where(usable, rr0, 1.0)) / jnp.sqrt(jnp.where(usable, n1, 1.0)), 1.0)
    v = s * x1
    z = s * (s * x2)
    vv = total(v * v)
    a = ratio(total(x0 * v), vv)
    q = ratio(total(z * v), vv)
    u = x0 - a * v
    w = z - q * v
    t = v - a * z
    uw = total(u * w)
    ww = total(w * w)
    g = ratio(uw, ww)
    b = u - g * w
    dots = [s, a, q, g, rr0, total(u * u), total(u * v), vv, total(u * t), uw, total(v * t), total(v * w),
            total(b * b), total(b * v), total(b * w), ww, total(b * t), total(w * t)]
    weight = jnp.where(mine, mass, 0.0)
    pairs = [(b, b), (b, v), (b, w), (v, v), (v, w), (w, w)]
    energy = [total(weight * (l * r)) for l, r in pairs]

    apply_elements(v2_ref, idx_ref, grads_ref, moduli_ref, s2_ref, None, rows)
    per = moduli_ref.shape[0] // 2

    def step(j, sums):
        at = j * 8
        lam = moduli_ref[pl.ds(at, 8), :]
        mu = moduli_ref[pl.ds(per + at, 8), :]
        e0, e1, e2 = [[ref[pl.ds(p * per + at, 8), :] for p in range(6)] for ref in (s0_ref, s1_ref, s2_ref)]
        ev = [s * e for e in e1]
        ew = [s * (s * e) - q * h for e, h in zip(e2, ev)]
        eb = [e - a * h - g * k for e, h, k in zip(e0, ev, ew)]
        tb, tv, tw = [stresses(e, lam, mu) for e in (eb, ev, ew)]
        new = [work(tb, eb), work(tb, ev), work(tb, ew), work(tv, ev), work(tv, ew), work(tw, ew)]
        return tuple(x + y for x, y in zip(sums, new))

    sums = lax.fori_loop(0, per // 8, step, (jnp.zeros((8, LANE), jnp.float32),) * 6)
    numbers = dots + [e + total(x) for e, x in zip(energy, sums)]
    lane = lax.broadcasted_iota(jnp.int32, (1, LANE), 1)
    lines_ = []
    for r in range(8):
        line = jnp.broadcast_to(numbers[r], (1, LANE))
        for i in range(r + 8, len(numbers), 8):
            line = jnp.where(lane < i // 8 * (LANE // 4), line, numbers[i])
        lines_.append(line)
    msg_ref[...] = jnp.broadcast_to(jnp.concatenate(lines_, axis=0)[None], msg_ref.shape)


def last_kernel(recv_ref, v0_ref, v1_ref, v2_ref, idx_ref, out_ref, table_ref, *, rows):
    size = recv_ref.shape[0]

    def number(i):
        at = i // 8 * (LANE // 4)
        return jnp.broadcast_to(recv_ref[:, i % 8, :][:, at : at + 1], (size, LANE))

    def over(x):
        return jnp.sum(x, axis=0, keepdims=True)

    (s, a, q, g, rr0, uu, uv, vv, ut, uw, vt, vw, bb, bv, bw, ww, bt, wt,
     ebb, ebv, ebw, evv, evw, eww) = [number(i) for i in range(24)]
    inv = 1.0 / s
    rr0 = over(rr0)
    curv0 = over(inv * (uv + a * vv))
    alpha0 = rr0 / curv0
    a0 = alpha0 * inv
    d = a - a0
    rr1 = over(uu + d * (2.0 * uv + d * vv))
    own1 = over(inv * (ut + d * (uw + q * uv + vt + d * (vw + q * vv))))
    cross1 = over(inv * (uv + d * vv))
    beta0 = rr1 / rr0
    curv1 = own1 + beta0 * (2.0 * cross1 + beta0 * curv0)
    alpha1 = rr1 / curv1
    a1 = alpha1 * inv
    c2 = a0 * a1
    m1 = g + c2
    m0 = a - a0 - a1 * (1.0 + beta0) + q * c2
    h = d * q + beta0
    rr2 = over(bb + m0 * (2.0 * bv + m0 * vv) + m1 * (2.0 * (bw + m0 * vw) + m1 * ww))
    cross2 = over(inv * (bt + d * bw + h * bv + m0 * (vt + d * vw + h * vv) + m1 * (wt + d * ww + h * vw)))
    own2 = over(ebb + m0 * (2.0 * ebv + m0 * evv) + m1 * (2.0 * (ebw + m0 * evw) + m1 * eww))
    beta1 = rr2 / rr1
    curv2 = own2 + beta1 * (2.0 * cross2 + beta1 * curv1)
    alpha2 = rr2 / curv2

    wide = lambda x: jnp.concatenate([x, x], axis=1)
    alpha0, alpha1, alpha2, beta0, beta1 = [wide(x) for x in (alpha0, alpha1, alpha2, beta0, beta1)]
    v0 = v0_ref[...]
    v1 = v1_ref[...]
    r1 = v0 - alpha0 * v1
    d1 = r1 + beta0 * v0
    image1 = (v1 - alpha0 * v2_ref[...]) + beta0 * v1
    r2 = r1 - alpha1 * image1
    d2 = r2 + beta1 * d1
    table_ref[...] = 0.5 * (alpha0 * v0 + alpha1 * d1 + alpha2 * d2)
    per = idx_ref.shape[0] // 2
    for j in range(per // 8):
        v = gather(table_ref, [idx_ref[k * per + j * 8 : k * per + j * 8 + 8, :] for k in range(2)], rows)
        for c in range(3):
            got = v[0][c] + v[1][c]
            for q in range(8):
                at = (j * 8 + q) * LANE
                out_ref[c : c + 1, at : at + LANE] = got[q : q + 1, :]


def call(kernel, args, outs, scratch=()):
    spaces = {"s": pltpu.SMEM, "v": pltpu.VMEM, "h": pltpu.VMEM}
    arrays = [pltpu.with_memory_space_constraint(x, pltpu.VMEM) if m == "v" else x for x, m in args]
    return pl.pallas_call(
        kernel,
        out_shape=[o for o, _ in outs],
        in_specs=[pl.BlockSpec(memory_space=spaces[m]) for _, m in args],
        out_specs=[pl.BlockSpec(memory_space=spaces[m]) for _, m in outs],
        scratch_shapes=list(scratch),
    )(*arrays)


def rotated(x, axis, by):
    n = lax.axis_size(axis)
    return lax.ppermute(x, axis, [(i, (i + by) % n) for i in range(n)])


def body(fine_res, node_map, connect, grads, moduli, mass):
    size = lax.axis_size("sub")
    groups = lax.axis_size("grp")
    own = mass.shape[0]
    fine = node_map.shape[1]
    elems = connect.shape[1]
    rows = (own + CI) // LO
    k = CI // LO
    col = lax.axis_index("sub").astype(jnp.int32).reshape(1)
    fcount = 2 * fine // LANE
    ecount = 4 * elems // LANE

    def kept(*shape, dtype=jnp.float32):
        return pltpu.VMEM(shape, dtype), "v"

    table = kept(3 * HP, LO)
    edge = kept(3 * k, LO)
    acc = pltpu.VMEM((LO, 9 * HP), jnp.float32)
    parts = pltpu.VMEM((9 * ecount, LANE), jnp.float32)
    strain = kept(6 * elems // LANE, LANE)
    mass2 = mass.reshape(own // LANE, LANE)

    partial, lower, upper, map_idx = call(
        functools.partial(rhs_kernel, own=own),
        [(col, "s"), (node_map, "h"), (fine_res, "h"), (mass2, "h")],
        [table, kept(4 * k, LO), edge, kept(fcount, LANE, dtype=jnp.int32)],
        [pltpu.VMEM((3 * fcount // 2, LANE), jnp.float32), pltpu.VMEM((9 * fcount, LANE), jnp.float32), acc],
    )
    before = rotated(upper, "sub", 1)
    after = rotated(lower, "sub", -1)
    idx, g, mod = call(
        functools.partial(prep_kernel, own=own),
        [(col, "s"), (connect, "h"), (grads, "h"), (moduli, "h")],
        [kept(ecount, LANE, dtype=jnp.int32), kept(9 * elems // LANE, LANE), kept(2 * elems // LANE, LANE)],
    )
    part, mass_ext = call(
        functools.partial(halo_kernel, own=own, size=size),
        [(col, "s"), (partial, "v"), (before, "v"), (after, "v"), (mass2, "h"), (mod, "v")],
        [table, kept(HP, LO)],
    )
    sums = [part] + [rotated(part, "grp", i) for i in range(1, groups)]
    elements = [(idx, "v"), (g, "v"), (mod, "v")]
    kw = dict(own=own, rows=rows)
    v0, f0, lower, upper, s0 = call(
        functools.partial(first_kernel, groups=groups, **kw),
        [(x, "v") for x in sums] + elements,
        [table, table, edge, edge, strain],
        [parts, acc],
    )
    before = rotated(upper, "sub", 1)
    after = rotated(lower, "sub", -1)
    v1, f1, lower, upper, s1 = call(
        functools.partial(second_kernel, size=size, **kw),
        [(col, "s"), (before, "v"), (after, "v"), (v0, "v"), (f0, "v"), (mass_ext, "v")] + elements,
        [table, table, edge, edge, strain],
        [parts, acc],
    )
    before = rotated(upper, "sub", 1)
    after = rotated(lower, "sub", -1)
    msg, v2 = call(
        functools.partial(third_kernel, size=size, **kw),
        [(col, "s")] + [(x, "v") for x in (before, after, v0, v1, f1, s0, s1, mass_ext)] + elements,
        [kept(size, 8, LANE), table],
        [pltpu.VMEM((6 * elems // LANE, LANE), jnp.float32)],
    )
    recv = lax.all_to_all(msg, "sub", 0, 0)
    (out,) = call(
        functools.partial(last_kernel, rows=rows),
        [(recv, "v"), (v0, "v"), (v1, "v"), (v2, "v"), (map_idx, "v")],
        [(jax.ShapeDtypeStruct((3, fine), jnp.float32), "h")],
        [pltpu.VMEM((3 * HP, LO), jnp.float32)],
    )
    return out


def solution(mesh):
    in_specs = (
        P(None, ("grp", "sub")),
        P(None, ("grp", "sub")),
        P(None, "sub"),
        P(None, None, "sub"),
        P(None, "sub"),
        P("sub"),
    )
    out_specs = P(None, ("grp", "sub"))
    return jax.shard_map(body, mesh=mesh, in_specs=in_specs, out_specs=out_specs, check_vma=False)
```

```python
import functools

import jax
import jax.numpy as jnp
from jax import lax
from jax.experimental import pallas as pl
from jax.experimental.pallas import tpu as pltpu
from jax.sharding import PartitionSpec as P

CI = 1024
LANE = 128
LO = 256
HP = 16
RC = 32

PAIRS = ((0, 0), (1, 1), (2, 2), (0, 1), (0, 2), (1, 2))
SYM = ((0, 3, 4), (3, 1, 5), (4, 5, 2))


def split3(x):
    a = x.astype(jnp.bfloat16).astype(jnp.float32)
    r = x - a
    b = r.astype(jnp.bfloat16).astype(jnp.float32)
    return a, b, r - b


def gather(table, idxs, rows):
    out = []
    for ix in idxs:
        lo = ix & (LANE - 1)
        hi = ix >> 7
        got = [jnp.zeros((8, LANE), jnp.float32)] * 3
        for h in range(rows * LO // LANE):
            r, half = divmod(h, LO // LANE)
            mask = hi == h
            for c in range(3):
                row = table[c * HP + r : c * HP + r + 1, half * LANE : (half + 1) * LANE]
                row = jnp.broadcast_to(row, (8, LANE))
                moved = jnp.take_along_axis(row, lo, axis=1, mode="promise_in_bounds")
                got[c] = jnp.where(mask, moved, got[c])
        out.append(got)
    return out


def scatter(idx_ref, cols_ref, parts_ref, acc_ref, count):
    hi_iota = lax.broadcasted_iota(jnp.int32, (HP, LANE), 0)
    lo_iota = lax.broadcasted_iota(jnp.int32, (LANE, LO), 1).astype(jnp.float32).astype(jnp.bfloat16)
    one = jnp.bfloat16(1)
    zero = jnp.bfloat16(0)
    acc_ref[...] = jnp.zeros(acc_ref.shape, jnp.float32)
    for i in range(count // RC):
        hot, moved = [], []
        for row in range(i * RC, i * RC + RC):
            lo = (cols_ref[:, row : row + 1] & (LO - 1)).astype(jnp.float32)
            lo = jnp.broadcast_to(lo, (LANE, LANE)).astype(jnp.bfloat16)
            hot.append(jnp.where(lo_iota == jnp.concatenate([lo, lo], axis=1), one, zero))
            mask = hi_iota == (idx_ref[row : row + 1, :] >> 8)
            group = [
                jnp.where(mask, parts_ref[p * count + row : p * count + row + 1, :], 0.0).astype(jnp.bfloat16)
                for p in range(9)
            ]
            moved.append(jnp.concatenate(group, axis=0))
        acc_ref[...] += lax.dot_general(
            jnp.concatenate(moved, axis=1),
            jnp.concatenate(hot, axis=0),
            (((1,), (0,)), ((), ())),
            preferred_element_type=jnp.float32,
        )
    n = 3 * HP
    return acc_ref[:n] + acc_ref[n : 2 * n] + acc_ref[2 * n :]


def lines(ref, lead, dst, base, f=lambda x: x):
    n = ref.shape[-1] // LANE
    for q in range(n):
        dst[base + q : base + q + 1, :] = f(ref[lead + (slice(q * LANE, (q + 1) * LANE),)])


def rhs_kernel(col_ref, map_ref, fine_ref, mass_ref, out_ref, one_ref, two_ref, idx_ref,
               half_ref, cols_ref, parts_ref, acc_ref, *, own):
    half = map_ref.shape[1] // LANE
    count = 2 * half
    shift = col_ref[0] * own
    for k in range(2):
        lines(map_ref, (slice(k, k + 1),), idx_ref, k * half, lambda x: x - shift)
    cols_ref[...] = jnp.transpose(idx_ref[...])
    for c in range(3):
        lines(fine_ref, (slice(c, c + 1),), half_ref, c * half)
    for c in range(3):
        pieces = split3(0.5 * half_ref[c * half : (c + 1) * half, :])
        for s in range(3):
            for k in range(2):
                at = (s * 3 + c) * count + k * half
                parts_ref[at : at + half, :] = pieces[s]
    table = scatter(idx_ref, cols_ref, parts_ref, acc_ref, count)
    out_ref[...] = table
    k = CI // LO
    lower, upper = shared(table, own)
    mass = jnp.concatenate([mass_ref[pl.ds(0, k, stride=2), :], mass_ref[pl.ds(1, k, stride=2), :]], axis=1)
    send(one_ref, two_ref, col_ref[0], jnp.concatenate([lower, mass], axis=0), jnp.concatenate([upper, mass], axis=0))


def prep_kernel(col_ref, conn_ref, grads_ref, moduli_ref, idx_ref, cols_ref, g_ref, m_ref, *, own):
    per = moduli_ref.shape[1] // LANE
    shift = col_ref[0] * own
    for a in range(4):
        lines(conn_ref, (slice(a, a + 1),), idx_ref, a * per, lambda x: x - shift)
    cols_ref[...] = jnp.transpose(idx_ref[...])
    for d in range(3):
        for a in range(3):
            lines(grads_ref, (d, slice(a, a + 1)), g_ref, (d * 3 + a) * per)
    for i in range(2):
        lines(moduli_ref, (slice(i, i + 1),), m_ref, i * per)


def shared(table, own):
    k = CI // LO
    base = own // LO
    lower = jnp.concatenate([table[c * HP : c * HP + k] for c in range(3)], axis=0)
    upper = jnp.concatenate([table[c * HP + base : c * HP + base + k] for c in range(3)], axis=0)
    return lower, upper


def send(one_ref, two_ref, col, lower, upper):
    even = col % 2 == 0
    one_ref[...] = jnp.where(even, upper, lower)
    two_ref[...] = jnp.where(even, lower, upper)


def received(one_ref, two_ref, col):
    even = col % 2 == 0
    one, two = one_ref[...], two_ref[...]
    return jnp.where(even, two, one), jnp.where(even, one, two)


def halo_kernel(col_ref, table_ref, one_ref, two_ref, mass_ref, moduli_ref, out_ref, mass_out_ref, *, own, size):
    col = col_ref[0]
    k = CI // LO
    before, after = received(one_ref, two_ref, col)
    out_ref[...] = add_halo(table_ref[...], col, before[: 3 * k], after[: 3 * k], own, size)
    mine = jnp.concatenate(
        [mass_ref[pl.ds(0, own // LO, stride=2), :], mass_ref[pl.ds(1, own // LO, stride=2), :]], axis=1
    )
    pad = jnp.zeros((HP - own // LO - k, LO), jnp.float32)
    mass_out_ref[...] = jnp.concatenate([mine, after[3 * k :], pad], axis=0)


def apply_elements(table, idx_ref, grads_ref, moduli_ref, strain_ref, parts_ref, rows):
    per = moduli_ref.shape[0] // 2
    count = 4 * per

    def step(j, carry):
        at = j * 8
        v = gather(table, [idx_ref[pl.ds(k * per + at, 8), :] for k in range(4)], rows)
        g = [[grads_ref[pl.ds((d * 3 + a) * per + at, 8), :] for d in range(3)] for a in range(3)]
        w = [[v[a][i] - v[3][i] for i in range(3)] for a in range(3)]
        grad = [[w[0][i] * g[0][j] + w[1][i] * g[1][j] + w[2][i] * g[2][j] for j in range(3)] for i in range(3)]
        strain = [0.5 * (grad[i][j] + grad[j][i]) for i, j in PAIRS]
        for p in range(6):
            strain_ref[pl.ds(p * per + at, 8), :] = strain[p]
        if parts_ref is not None:
            lam = moduli_ref[pl.ds(at, 8), :]
            mu = moduli_ref[pl.ds(per + at, 8), :]
            stress = stresses(strain, lam, mu)
            for i in range(3):
                f = [sum(stress[SYM[i][j]] * g[a][j] for j in range(3)) for a in range(3)]
                f.append(-(f[0] + f[1] + f[2]))
                for a in range(4):
                    pieces = split3(f[a])
                    for s in range(3):
                        parts_ref[pl.ds((s * 3 + i) * count + a * per + at, 8), :] = pieces[s]
        return carry

    lax.fori_loop(0, per // 8, step, 0)


def stresses(strain, lam, mu):
    bulk = lam * (strain[0] + strain[1] + strain[2])
    return [2.0 * mu * strain[p] + (bulk if p < 3 else 0.0) for p in range(6)]


def work(stress, strain):
    diag = stress[0] * strain[0] + stress[1] * strain[1] + stress[2] * strain[2]
    return diag + 2.0 * (stress[3] * strain[3] + stress[4] * strain[4] + stress[5] * strain[5])


def own_rows(own):
    r = lax.broadcasted_iota(jnp.int32, (3 * HP, LO), 0) & (HP - 1)
    return r < own // LO


def per_component(x):
    return jnp.concatenate([x, x, x], axis=0)


def add_halo(own_part, col, down, up, own, size):
    k = CI // LO
    down = jnp.where(col > 0, down, 0.0)
    up = jnp.where(col < size - 1, up, 0.0)
    pieces = []
    for c in range(3):
        pieces.append(down[c * k : (c + 1) * k])
        pieces.append(jnp.zeros((own // LO - k, LO), jnp.float32))
        pieces.append(up[c * k : (c + 1) * k])
        pieces.append(jnp.zeros((HP - own // LO - k, LO), jnp.float32))
    return own_part + jnp.concatenate(pieces, axis=0)


def first_kernel(col_ref, *refs, own, rows, groups):
    sum_refs = refs[:groups]
    (idx_ref, cols_ref, grads_ref, moduli_ref, v_ref, f_ref, one_ref, two_ref, strain_ref, parts_ref,
     acc_ref) = refs[groups:]
    total = sum_refs[0][...]
    for ref in sum_refs[1:]:
        total = total + ref[...]
    v_ref[...] = total
    apply_elements(v_ref, idx_ref, grads_ref, moduli_ref, strain_ref, parts_ref, rows)
    f = scatter(idx_ref, cols_ref, parts_ref, acc_ref, idx_ref.shape[0])
    f_ref[...] = f
    send(one_ref, two_ref, col_ref[0], *shared(f, own))


def second_kernel(col_ref, one_ref, two_ref, v0_ref, f0_ref, mass_ref, idx_ref, cols_ref, grads_ref, moduli_ref,
                  v_ref, f_ref, one_out_ref, two_out_ref, strain_ref, parts_ref, acc_ref, *, own, rows, size):
    mass = per_component(mass_ref[...])
    before, after = received(one_ref, two_ref, col_ref[0])
    v_ref[...] = add_halo(f0_ref[...] + mass * v0_ref[...], col_ref[0], before, after, own, size)
    apply_elements(v_ref, idx_ref, grads_ref, moduli_ref, strain_ref, parts_ref, rows)
    f = scatter(idx_ref, cols_ref, parts_ref, acc_ref, idx_ref.shape[0])
    f_ref[...] = f
    send(one_out_ref, two_out_ref, col_ref[0], *shared(f, own))


def total(x):
    return jnp.sum(x, axis=(0, 1), keepdims=True)


def ratio(a, b):
    return jnp.where(b > 0.0, a / jnp.where(b > 0.0, b, 1.0), 0.0)


def third_kernel(col_ref, one_ref, two_ref, v0_ref, v1_ref, f1_ref, s0_ref, s1_ref, mass_ref, idx_ref,
                 grads_ref, moduli_ref, msg_ref, v2_ref, s2_ref, *, own, rows, size):
    mass = per_component(mass_ref[...])
    before, after = received(one_ref, two_ref, col_ref[0])
    v2 = add_halo(f1_ref[...] + mass * v1_ref[...], col_ref[0], before, after, own, size)
    v2_ref[...] = v2
    mine = own_rows(own)
    x0 = jnp.where(mine, v0_ref[...], 0.0)
    x1 = jnp.where(mine, v1_ref[...], 0.0)
    x2 = jnp.where(mine, v2, 0.0)
    rr0 = total(x0 * x0)
    n1 = total(x1 * x1)
    usable = (rr0 > 0.0) & (n1 > 0.0)
    s = jnp.where(usable, jnp.sqrt(jnp.where(usable, rr0, 1.0)) / jnp.sqrt(jnp.where(usable, n1, 1.0)), 1.0)
    v = s * x1
    z = s * (s * x2)
    vv = total(v * v)
    a = ratio(total(x0 * v), vv)
    q = ratio(total(z * v), vv)
    u = x0 - a * v
    w = z - q * v
    t = v - a * z
    uw = total(u * w)
    ww = total(w * w)
    g = ratio(uw, ww)
    b = u - g * w
    dots = [s, a, q, g, rr0, total(u * u), total(u * v), vv, total(u * t), uw, total(v * t), total(v * w),
            total(b * b), total(b * v), total(b * w), ww, total(b * t), total(w * t)]
    weight = jnp.where(mine, mass, 0.0)
    pairs = [(b, b), (b, v), (b, w), (v, v), (v, w), (w, w)]
    energy = [total(weight * (l * r)) for l, r in pairs]

    apply_elements(v2_ref, idx_ref, grads_ref, moduli_ref, s2_ref, None, rows)
    per = moduli_ref.shape[0] // 2

    def step(j, sums):
        at = j * 8
        lam = moduli_ref[pl.ds(at, 8), :]
        mu = moduli_ref[pl.ds(per + at, 8), :]
        e0, e1, e2 = [[ref[pl.ds(p * per + at, 8), :] for p in range(6)] for ref in (s0_ref, s1_ref, s2_ref)]
        ev = [s * e for e in e1]
        ew = [s * (s * e) - q * h for e, h in zip(e2, ev)]
        eb = [e - a * h - g * k for e, h, k in zip(e0, ev, ew)]
        tb, tv, tw = [stresses(e, lam, mu) for e in (eb, ev, ew)]
        new = [work(tb, eb), work(tb, ev), work(tb, ew), work(tv, ev), work(tv, ew), work(tw, ew)]
        return tuple(x + y for x, y in zip(sums, new))

    sums = lax.fori_loop(0, per // 8, step, (jnp.zeros((8, LANE), jnp.float32),) * 6)
    numbers = dots + [e + total(x) for e, x in zip(energy, sums)]
    lane = lax.broadcasted_iota(jnp.int32, (1, LANE), 1)
    lines_ = []
    for r in range(8):
        line = jnp.broadcast_to(numbers[r], (1, LANE))
        for i in range(r + 8, len(numbers), 8):
            line = jnp.where(lane < i // 8 * (LANE // 4), line, numbers[i])
        lines_.append(line)
    msg_ref[...] = jnp.broadcast_to(jnp.concatenate(lines_, axis=0)[None], msg_ref.shape)


def last_kernel(recv_ref, v0_ref, v1_ref, v2_ref, idx_ref, out_ref, table_ref, *, rows):
    size = recv_ref.shape[0]

    def number(i):
        at = i // 8 * (LANE // 4)
        return jnp.broadcast_to(recv_ref[:, i % 8, :][:, at : at + 1], (size, LANE))

    def over(x):
        return jnp.sum(x, axis=0, keepdims=True)

    (s, a, q, g, rr0, uu, uv, vv, ut, uw, vt, vw, bb, bv, bw, ww, bt, wt,
     ebb, ebv, ebw, evv, evw, eww) = [number(i) for i in range(24)]
    inv = 1.0 / s
    rr0 = over(rr0)
    curv0 = over(inv * (uv + a * vv))
    alpha0 = rr0 / curv0
    a0 = alpha0 * inv
    d = a - a0
    rr1 = over(uu + d * (2.0 * uv + d * vv))
    own1 = over(inv * (ut + d * (uw + q * uv + vt + d * (vw + q * vv))))
    cross1 = over(inv * (uv + d * vv))
    beta0 = rr1 / rr0
    curv1 = own1 + beta0 * (2.0 * cross1 + beta0 * curv0)
    alpha1 = rr1 / curv1
    a1 = alpha1 * inv
    c2 = a0 * a1
    m1 = g + c2
    m0 = a - a0 - a1 * (1.0 + beta0) + q * c2
    h = d * q + beta0
    rr2 = over(bb + m0 * (2.0 * bv + m0 * vv) + m1 * (2.0 * (bw + m0 * vw) + m1 * ww))
    cross2 = over(inv * (bt + d * bw + h * bv + m0 * (vt + d * vw + h * vv) + m1 * (wt + d * ww + h * vw)))
    own2 = over(ebb + m0 * (2.0 * ebv + m0 * evv) + m1 * (2.0 * (ebw + m0 * evw) + m1 * eww))
    beta1 = rr2 / rr1
    curv2 = own2 + beta1 * (2.0 * cross2 + beta1 * curv1)
    alpha2 = rr2 / curv2

    wide = lambda x: jnp.concatenate([x, x], axis=1)
    alpha0, alpha1, alpha2, beta0, beta1 = [wide(x) for x in (alpha0, alpha1, alpha2, beta0, beta1)]
    v0 = v0_ref[...]
    v1 = v1_ref[...]
    r1 = v0 - alpha0 * v1
    d1 = r1 + beta0 * v0
    image1 = (v1 - alpha0 * v2_ref[...]) + beta0 * v1
    r2 = r1 - alpha1 * image1
    d2 = r2 + beta1 * d1
    table_ref[...] = 0.5 * (alpha0 * v0 + alpha1 * d1 + alpha2 * d2)
    per = idx_ref.shape[0] // 2
    for j in range(per // 8):
        v = gather(table_ref, [idx_ref[k * per + j * 8 : k * per + j * 8 + 8, :] for k in range(2)], rows)
        for c in range(3):
            got = v[0][c] + v[1][c]
            for q in range(8):
                at = (j * 8 + q) * LANE
                out_ref[c : c + 1, at : at + LANE] = got[q : q + 1, :]


def call(kernel, args, outs, scratch=()):
    spaces = {"s": pltpu.SMEM, "v": pltpu.VMEM, "h": pltpu.VMEM}
    arrays = [pltpu.with_memory_space_constraint(x, pltpu.VMEM) if m == "v" else x for x, m in args]
    return pl.pallas_call(
        kernel,
        out_shape=[o for o, _ in outs],
        in_specs=[pl.BlockSpec(memory_space=spaces[m]) for _, m in args],
        out_specs=[pl.BlockSpec(memory_space=spaces[m]) for _, m in outs],
        scratch_shapes=list(scratch),
    )(*arrays)


def rotated(x, axis, by):
    n = lax.axis_size(axis)
    return lax.ppermute(x, axis, [(i, (i + by) % n) for i in range(n)])


def traded(one, two):
    size = lax.axis_size("sub")
    groups = lax.axis_size("grp")
    outs = []
    for x, first in ((one, 0), (two, 1)):
        pairs = []
        for g in range(groups):
            for c in range(size):
                other = c + 1 if c % 2 == first else c - 1
                if 0 <= other < size:
                    pairs.append((g * size + c, g * size + other))
                else:
                    pairs.append((g * size + c, (g ^ 1) * size + c))
        outs.append(lax.ppermute(x, ("grp", "sub"), pairs))
    return outs


def body(fine_res, node_map, connect, grads, moduli, mass):
    size = lax.axis_size("sub")
    groups = lax.axis_size("grp")
    own = mass.shape[0]
    fine = node_map.shape[1]
    elems = connect.shape[1]
    rows = (own + CI) // LO
    k = CI // LO
    col = lax.axis_index("sub").astype(jnp.int32).reshape(1)
    fcount = 2 * fine // LANE
    ecount = 4 * elems // LANE

    def kept(*shape, dtype=jnp.float32):
        return pltpu.VMEM(shape, dtype), "v"

    table = kept(3 * HP, LO)
    edge = kept(3 * k, LO)
    acc = pltpu.VMEM((9 * HP, LO), jnp.float32)
    parts = pltpu.VMEM((9 * ecount, LANE), jnp.float32)
    strain = kept(6 * elems // LANE, LANE)
    mass2 = mass.reshape(own // LANE, LANE)

    partial, one, two, map_idx = call(
        functools.partial(rhs_kernel, own=own),
        [(col, "s"), (node_map, "h"), (fine_res, "h"), (mass2, "h")],
        [table, kept(4 * k, LO), kept(4 * k, LO), kept(fcount, LANE, dtype=jnp.int32)],
        [pltpu.VMEM((3 * fcount // 2, LANE), jnp.float32), pltpu.VMEM((LANE, fcount), jnp.int32),
         pltpu.VMEM((9 * fcount, LANE), jnp.float32), acc],
    )
    one, two = traded(one, two)
    idx, cols, g, mod = call(
        functools.partial(prep_kernel, own=own),
        [(col, "s"), (connect, "h"), (grads, "h"), (moduli, "h")],
        [kept(ecount, LANE, dtype=jnp.int32), kept(LANE, ecount, dtype=jnp.int32), kept(9 * elems // LANE, LANE), kept(2 * elems // LANE, LANE)],
    )
    part, mass_ext = call(
        functools.partial(halo_kernel, own=own, size=size),
        [(col, "s"), (partial, "v"), (one, "v"), (two, "v"), (mass2, "h"), (mod, "v")],
        [table, kept(HP, LO)],
    )
    sums = [part] + [rotated(part, "grp", i) for i in range(1, groups)]
    elements = [(idx, "v"), (g, "v"), (mod, "v")]
    summing = [(idx, "v"), (cols, "v"), (g, "v"), (mod, "v")]
    kw = dict(own=own, rows=rows)
    v0, f0, one, two, s0 = call(
        functools.partial(first_kernel, groups=groups, **kw),
        [(col, "s")] + [(x, "v") for x in sums] + summing,
        [table, table, edge, edge, strain],
        [parts, acc],
    )
    one, two = traded(one, two)
    v1, f1, one, two, s1 = call(
        functools.partial(second_kernel, size=size, **kw),
        [(col, "s"), (one, "v"), (two, "v"), (v0, "v"), (f0, "v"), (mass_ext, "v")] + summing,
        [table, table, edge, edge, strain],
        [parts, acc],
    )
    one, two = traded(one, two)
    msg, v2 = call(
        functools.partial(third_kernel, size=size, **kw),
        [(col, "s")] + [(x, "v") for x in (one, two, v0, v1, f1, s0, s1, mass_ext)] + elements,
        [kept(size, 8, LANE), table],
        [pltpu.VMEM((6 * elems // LANE, LANE), jnp.float32)],
    )
    recv = lax.all_to_all(msg, "sub", 0, 0)
    (out,) = call(
        functools.partial(last_kernel, rows=rows),
        [(recv, "v"), (v0, "v"), (v1, "v"), (v2, "v"), (map_idx, "v")],
        [(jax.ShapeDtypeStruct((3, fine), jnp.float32), "h")],
        [pltpu.VMEM((3 * HP, LO), jnp.float32)],
    )
    return out


def solution(mesh):
    in_specs = (
        P(None, ("grp", "sub")),
        P(None, ("grp", "sub")),
        P(None, "sub"),
        P(None, None, "sub"),
        P(None, "sub"),
        P("sub"),
    )
    out_specs = P(None, ("grp", "sub"))
    return jax.shard_map(body, mesh=mesh, in_specs=in_specs, out_specs=out_specs, check_vma=False)
```

```python
import functools

import jax
import jax.numpy as jnp
from jax import lax
from jax.experimental import pallas as pl
from jax.experimental.pallas import tpu as pltpu
from jax.sharding import PartitionSpec as P

CI = 1024
LANE = 128
LO = 256
HP = 16
ROOM = 16 << 20
RC = 32

PAIRS = ((0, 0), (1, 1), (2, 2), (0, 1), (0, 2), (1, 2))
SYM = ((0, 3, 4), (3, 1, 5), (4, 5, 2))


def split3(x):
    a = x.astype(jnp.bfloat16).astype(jnp.float32)
    r = x - a
    b = r.astype(jnp.bfloat16).astype(jnp.float32)
    return a, b, r - b


def gather(table, idxs, rows):
    out = []
    for ix in idxs:
        lo = ix & (LANE - 1)
        hi = ix >> 7
        got = [jnp.zeros((8, LANE), jnp.float32)] * 3
        for h in range(rows * LO // LANE):
            r, half = divmod(h, LO // LANE)
            mask = hi == h
            for c in range(3):
                row = table[c * HP + r : c * HP + r + 1, half * LANE : (half + 1) * LANE]
                row = jnp.broadcast_to(row, (8, LANE))
                moved = jnp.take_along_axis(row, lo, axis=1, mode="promise_in_bounds")
                got[c] = jnp.where(mask, moved, got[c])
        out.append(got)
    return out


def scatter(idx_ref, cols_ref, parts_ref, acc_ref, count):
    hi_iota = lax.broadcasted_iota(jnp.int32, (HP, LANE), 0)
    lo_iota = lax.broadcasted_iota(jnp.int32, (LANE, LO), 1).astype(jnp.float32).astype(jnp.bfloat16)
    one = jnp.bfloat16(1)
    zero = jnp.bfloat16(0)
    acc_ref[...] = jnp.zeros(acc_ref.shape, jnp.float32)
    for i in range(count // RC):
        hot, moved = [], []
        for row in range(i * RC, i * RC + RC):
            lo = (cols_ref[:, row : row + 1] & (LO - 1)).astype(jnp.float32)
            lo = jnp.broadcast_to(lo, (LANE, LANE)).astype(jnp.bfloat16)
            hot.append(jnp.where(lo_iota == jnp.concatenate([lo, lo], axis=1), one, zero))
            mask = hi_iota == (idx_ref[row : row + 1, :] >> 8)
            group = [
                jnp.where(mask, parts_ref[p * count + row : p * count + row + 1, :], 0.0).astype(jnp.bfloat16)
                for p in range(9)
            ]
            moved.append(jnp.concatenate(group, axis=0))
        acc_ref[...] += lax.dot_general(
            jnp.concatenate(moved, axis=1),
            jnp.concatenate(hot, axis=0),
            (((1,), (0,)), ((), ())),
            preferred_element_type=jnp.float32,
        )
    n = 3 * HP
    return acc_ref[:n] + acc_ref[n : 2 * n] + acc_ref[2 * n :]


def lines(ref, lead, dst, base, f=lambda x: x, group=8):
    n = ref.shape[-1] // LANE
    for q in range(n):
        to = base + q // 8 * group + q % 8
        dst[to : to + 1, :] = f(ref[lead + (slice(q * LANE, (q + 1) * LANE),)])


def rhs_kernel(col_ref, map_ref, fine_ref, mass_ref, out_ref, one_ref, two_ref, idx_ref,
               half_ref, cols_ref, parts_ref, acc_ref, *, own):
    half = map_ref.shape[1] // LANE
    count = 2 * half
    shift = col_ref[0] * own
    for k in range(2):
        lines(map_ref, (slice(k, k + 1),), idx_ref, k * half, lambda x: x - shift)
    cols_ref[...] = jnp.transpose(idx_ref[...])
    for c in range(3):
        lines(fine_ref, (slice(c, c + 1),), half_ref, c * half)
    for c in range(3):
        pieces = split3(0.5 * half_ref[c * half : (c + 1) * half, :])
        for s in range(3):
            for k in range(2):
                at = (s * 3 + c) * count + k * half
                parts_ref[at : at + half, :] = pieces[s]
    table = scatter(idx_ref, cols_ref, parts_ref, acc_ref, count)
    out_ref[...] = table
    k = CI // LO
    lower, upper = shared(table, own)
    mass = jnp.concatenate([mass_ref[pl.ds(0, k, stride=2), :], mass_ref[pl.ds(1, k, stride=2), :]], axis=1)
    send(one_ref, two_ref, col_ref[0], jnp.concatenate([lower, mass], axis=0), jnp.concatenate([upper, mass], axis=0))


def prep_kernel(col_ref, conn_ref, grads_ref, moduli_ref, idx_ref, cols_ref, g_ref, m_ref, *, own):
    per = moduli_ref.shape[1] // LANE
    shift = col_ref[0] * own
    for a in range(4):
        lines(conn_ref, (slice(a, a + 1),), idx_ref, a * 8, lambda x: x - shift, 32)
    cols_ref[...] = jnp.transpose(idx_ref[...])
    for d in range(3):
        for a in range(3):
            lines(grads_ref, (d, slice(a, a + 1)), g_ref, (d * 3 + a) * per)
    for i in range(2):
        lines(moduli_ref, (slice(i, i + 1),), m_ref, i * per)


def hot_kernel(cols_ref, hot_ref):
    lo_iota = lax.broadcasted_iota(jnp.int32, (LANE, LO), 1).astype(jnp.float32).astype(jnp.bfloat16)
    for row in range(cols_ref.shape[1]):
        lo = (cols_ref[:, row : row + 1] & (LO - 1)).astype(jnp.float32)
        lo = jnp.broadcast_to(lo, (LANE, LANE)).astype(jnp.bfloat16)
        hit = lo_iota == jnp.concatenate([lo, lo], axis=1)
        hot_ref[row * LANE : (row + 1) * LANE, :] = jnp.where(hit, jnp.bfloat16(1), jnp.bfloat16(0))


def shared(table, own):
    k = CI // LO
    base = own // LO
    lower = jnp.concatenate([table[c * HP : c * HP + k] for c in range(3)], axis=0)
    upper = jnp.concatenate([table[c * HP + base : c * HP + base + k] for c in range(3)], axis=0)
    return lower, upper


def send(one_ref, two_ref, col, lower, upper):
    even = col % 2 == 0
    one_ref[...] = jnp.where(even, upper, lower)
    two_ref[...] = jnp.where(even, lower, upper)


def received(one_ref, two_ref, col):
    even = col % 2 == 0
    one, two = one_ref[...], two_ref[...]
    return jnp.where(even, two, one), jnp.where(even, one, two)


def halo_kernel(col_ref, table_ref, one_ref, two_ref, mass_ref, moduli_ref, out_ref, mass_out_ref, *, own, size):
    col = col_ref[0]
    k = CI // LO
    before, after = received(one_ref, two_ref, col)
    out_ref[...] = add_halo(table_ref[...], col, before[: 3 * k], after[: 3 * k], own, size)
    mine = jnp.concatenate(
        [mass_ref[pl.ds(0, own // LO, stride=2), :], mass_ref[pl.ds(1, own // LO, stride=2), :]], axis=1
    )
    pad = jnp.zeros((HP - own // LO - k, LO), jnp.float32)
    mass_out_ref[...] = jnp.concatenate([mine, after[3 * k :], pad], axis=0)


def element_strains(table, idx_ref, grads_ref, strain_ref, j, rows):
    per = grads_ref.shape[0] // 9
    at = j * 8
    v = gather(table, [idx_ref[j * 32 + k * 8 : j * 32 + k * 8 + 8, :] for k in range(4)], rows)
    g = [[grads_ref[(d * 3 + a) * per + at : (d * 3 + a) * per + at + 8, :] for d in range(3)] for a in range(3)]
    w = [[v[a][i] - v[3][i] for i in range(3)] for a in range(3)]
    grad = [[w[0][i] * g[0][j] + w[1][i] * g[1][j] + w[2][i] * g[2][j] for j in range(3)] for i in range(3)]
    strain = [0.5 * (grad[i][j] + grad[j][i]) for i, j in PAIRS]
    for p in range(6):
        strain_ref[p * per + at : p * per + at + 8, :] = strain[p]
    return strain, g


def apply_elements(table, idx_ref, hot_ref, grads_ref, moduli_ref, strain_ref, parts_ref, rows):
    per = moduli_ref.shape[0] // 2
    count = 4 * per
    hi_iota = lax.broadcasted_iota(jnp.int32, (HP, LANE), 0)
    acc = jnp.zeros((9 * HP, LO), jnp.float32)

    def forces(j):
        at = j * 8
        strain, g = element_strains(table, idx_ref, grads_ref, strain_ref, j, rows)
        stress = stresses(strain, moduli_ref[at : at + 8, :], moduli_ref[per + at : per + at + 8, :])
        for i in range(3):
            f = [sum(stress[SYM[i][j]] * g[a][j] for j in range(3)) for a in range(3)]
            f.append(-(f[0] + f[1] + f[2]))
            for a in range(4):
                pieces = split3(f[a])
                for s in range(3):
                    to = (s * 3 + i) * count + j * 32 + a * 8
                    parts_ref[to : to + 8, :] = pieces[s]

    def summed(j, acc):
        moved = []
        for row in range(j * 32, j * 32 + 32):
            mask = hi_iota == (idx_ref[row : row + 1, :] >> 8)
            group = [
                jnp.where(mask, parts_ref[p * count + row : p * count + row + 1, :], 0.0).astype(jnp.bfloat16)
                for p in range(9)
            ]
            moved.append(jnp.concatenate(group, axis=0))
        return acc + jnp.dot(
            jnp.concatenate(moved, axis=1),
            hot_ref[j * 32 * LANE : (j + 1) * 32 * LANE, :],
            preferred_element_type=jnp.float32,
        )

    for j in range(per // 8 + 1):
        if j < per // 8:
            forces(j)
        if j > 0:
            acc = summed(j - 1, acc)
    n = 3 * HP
    return acc[:n] + acc[n : 2 * n] + acc[2 * n :]


def stresses(strain, lam, mu):
    bulk = lam * (strain[0] + strain[1] + strain[2])
    return [2.0 * mu * strain[p] + (bulk if p < 3 else 0.0) for p in range(6)]


def work(stress, strain):
    diag = stress[0] * strain[0] + stress[1] * strain[1] + stress[2] * strain[2]
    return diag + 2.0 * (stress[3] * strain[3] + stress[4] * strain[4] + stress[5] * strain[5])


def own_rows(own):
    r = lax.broadcasted_iota(jnp.int32, (3 * HP, LO), 0) & (HP - 1)
    return r < own // LO


def per_component(x):
    return jnp.concatenate([x, x, x], axis=0)


def add_halo(own_part, col, down, up, own, size):
    k = CI // LO
    down = jnp.where(col > 0, down, 0.0)
    up = jnp.where(col < size - 1, up, 0.0)
    pieces = []
    for c in range(3):
        pieces.append(down[c * k : (c + 1) * k])
        pieces.append(jnp.zeros((own // LO - k, LO), jnp.float32))
        pieces.append(up[c * k : (c + 1) * k])
        pieces.append(jnp.zeros((HP - own // LO - k, LO), jnp.float32))
    return own_part + jnp.concatenate(pieces, axis=0)


def first_kernel(col_ref, *refs, own, rows, groups):
    sum_refs = refs[:groups]
    idx_ref, hot_ref, grads_ref, moduli_ref, v_ref, f_ref, one_ref, two_ref, strain_ref, parts_ref = refs[groups:]
    total = sum_refs[0][...]
    for ref in sum_refs[1:]:
        total = total + ref[...]
    v_ref[...] = total
    f = apply_elements(v_ref, idx_ref, hot_ref, grads_ref, moduli_ref, strain_ref, parts_ref, rows)
    f_ref[...] = f
    send(one_ref, two_ref, col_ref[0], *shared(f, own))


def second_kernel(col_ref, one_ref, two_ref, v0_ref, f0_ref, mass_ref, idx_ref, hot_ref, grads_ref, moduli_ref,
                  v_ref, f_ref, one_out_ref, two_out_ref, strain_ref, parts_ref, *, own, rows, size):
    mass = per_component(mass_ref[...])
    before, after = received(one_ref, two_ref, col_ref[0])
    v_ref[...] = add_halo(f0_ref[...] + mass * v0_ref[...], col_ref[0], before, after, own, size)
    f = apply_elements(v_ref, idx_ref, hot_ref, grads_ref, moduli_ref, strain_ref, parts_ref, rows)
    f_ref[...] = f
    send(one_out_ref, two_out_ref, col_ref[0], *shared(f, own))


def total(x):
    return jnp.sum(x, axis=(0, 1), keepdims=True)


def ratio(a, b):
    return jnp.where(b > 0.0, a / jnp.where(b > 0.0, b, 1.0), 0.0)


def third_kernel(col_ref, one_ref, two_ref, v0_ref, v1_ref, f1_ref, s0_ref, s1_ref, mass_ref, idx_ref,
                 grads_ref, moduli_ref, msg_ref, v2_ref, s2_ref, *, own, rows, size):
    mass = per_component(mass_ref[...])
    before, after = received(one_ref, two_ref, col_ref[0])
    v2 = add_halo(f1_ref[...] + mass * v1_ref[...], col_ref[0], before, after, own, size)
    v2_ref[...] = v2
    mine = own_rows(own)
    x0 = jnp.where(mine, v0_ref[...], 0.0)
    x1 = jnp.where(mine, v1_ref[...], 0.0)
    x2 = jnp.where(mine, v2, 0.0)
    rr0 = total(x0 * x0)
    n1 = total(x1 * x1)
    usable = (rr0 > 0.0) & (n1 > 0.0)
    s = jnp.where(usable, jnp.sqrt(jnp.where(usable, rr0, 1.0)) / jnp.sqrt(jnp.where(usable, n1, 1.0)), 1.0)
    v = s * x1
    z = s * (s * x2)
    vv = total(v * v)
    a = ratio(total(x0 * v), vv)
    q = ratio(total(z * v), vv)
    u = x0 - a * v
    w = z - q * v
    t = v - a * z
    uw = total(u * w)
    ww = total(w * w)
    g = ratio(uw, ww)
    b = u - g * w
    dots = [s, a, q, g, rr0, total(u * u), total(u * v), vv, total(u * t), uw, total(v * t), total(v * w),
            total(b * b), total(b * v), total(b * w), ww, total(b * t), total(w * t)]
    weight = jnp.where(mine, mass, 0.0)
    pairs = [(b, b), (b, v), (b, w), (v, v), (v, w), (w, w)]
    energy = [total(weight * (l * r)) for l, r in pairs]

    per = moduli_ref.shape[0] // 2
    for j in range(per // 8):
        element_strains(v2_ref, idx_ref, grads_ref, s2_ref, j, rows)

    def step(j, sums):
        at = j * 8
        lam = moduli_ref[at : at + 8, :]
        mu = moduli_ref[per + at : per + at + 8, :]
        e0, e1, e2 = [[ref[p * per + at : p * per + at + 8, :] for p in range(6)] for ref in (s0_ref, s1_ref, s2_ref)]
        ev = [s * e for e in e1]
        ew = [s * (s * e) - q * h for e, h in zip(e2, ev)]
        eb = [e - a * h - g * k for e, h, k in zip(e0, ev, ew)]
        tb, tv, tw = [stresses(e, lam, mu) for e in (eb, ev, ew)]
        new = [work(tb, eb), work(tb, ev), work(tb, ew), work(tv, ev), work(tv, ew), work(tw, ew)]
        return tuple(x + y for x, y in zip(sums, new))

    sums = (jnp.zeros((8, LANE), jnp.float32),) * 6
    for j in range(per // 8):
        sums = step(j, sums)
    numbers = dots + [e + total(x) for e, x in zip(energy, sums)]
    lane = lax.broadcasted_iota(jnp.int32, (1, LANE), 1)
    lines_ = []
    for r in range(8):
        line = jnp.broadcast_to(numbers[r], (1, LANE))
        for i in range(r + 8, len(numbers), 8):
            line = jnp.where(lane < i // 8 * (LANE // 4), line, numbers[i])
        lines_.append(line)
    msg_ref[...] = jnp.broadcast_to(jnp.concatenate(lines_, axis=0)[None], msg_ref.shape)


def last_kernel(recv_ref, v0_ref, v1_ref, v2_ref, idx_ref, out_ref, table_ref, *, rows):
    size = recv_ref.shape[0]

    def number(i):
        at = i // 8 * (LANE // 4)
        return jnp.broadcast_to(recv_ref[:, i % 8, :][:, at : at + 1], (size, LANE))

    def over(x):
        return jnp.sum(x, axis=0, keepdims=True)

    (s, a, q, g, rr0, uu, uv, vv, ut, uw, vt, vw, bb, bv, bw, ww, bt, wt,
     ebb, ebv, ebw, evv, evw, eww) = [number(i) for i in range(24)]
    inv = 1.0 / s
    rr0 = over(rr0)
    curv0 = over(inv * (uv + a * vv))
    alpha0 = rr0 / curv0
    a0 = alpha0 * inv
    d = a - a0
    rr1 = over(uu + d * (2.0 * uv + d * vv))
    own1 = over(inv * (ut + d * (uw + q * uv + vt + d * (vw + q * vv))))
    cross1 = over(inv * (uv + d * vv))
    beta0 = rr1 / rr0
    curv1 = own1 + beta0 * (2.0 * cross1 + beta0 * curv0)
    alpha1 = rr1 / curv1
    a1 = alpha1 * inv
    c2 = a0 * a1
    m1 = g + c2
    m0 = a - a0 - a1 * (1.0 + beta0) + q * c2
    h = d * q + beta0
    rr2 = over(bb + m0 * (2.0 * bv + m0 * vv) + m1 * (2.0 * (bw + m0 * vw) + m1 * ww))
    cross2 = over(inv * (bt + d * bw + h * bv + m0 * (vt + d * vw + h * vv) + m1 * (wt + d * ww + h * vw)))
    own2 = over(ebb + m0 * (2.0 * ebv + m0 * evv) + m1 * (2.0 * (ebw + m0 * evw) + m1 * eww))
    beta1 = rr2 / rr1
    curv2 = own2 + beta1 * (2.0 * cross2 + beta1 * curv1)
    alpha2 = rr2 / curv2

    wide = lambda x: jnp.concatenate([x, x], axis=1)
    alpha0, alpha1, alpha2, beta0, beta1 = [wide(x) for x in (alpha0, alpha1, alpha2, beta0, beta1)]
    v0 = v0_ref[...]
    v1 = v1_ref[...]
    r1 = v0 - alpha0 * v1
    d1 = r1 + beta0 * v0
    image1 = (v1 - alpha0 * v2_ref[...]) + beta0 * v1
    r2 = r1 - alpha1 * image1
    d2 = r2 + beta1 * d1
    table_ref[...] = 0.5 * (alpha0 * v0 + alpha1 * d1 + alpha2 * d2)
    per = idx_ref.shape[0] // 2
    for j in range(per // 8):
        v = gather(table_ref, [idx_ref[k * per + j * 8 : k * per + j * 8 + 8, :] for k in range(2)], rows)
        for c in range(3):
            got = v[0][c] + v[1][c]
            for q in range(8):
                at = (j * 8 + q) * LANE
                out_ref[c : c + 1, at : at + LANE] = got[q : q + 1, :]


def call(kernel, args, outs, scratch=(), limit=None):
    spaces = {"s": pltpu.SMEM, "v": pltpu.VMEM, "h": pltpu.VMEM}
    arrays = [pltpu.with_memory_space_constraint(x, pltpu.VMEM) if m == "v" else x for x, m in args]
    return pl.pallas_call(
        kernel,
        out_shape=[o for o, _ in outs],
        in_specs=[pl.BlockSpec(memory_space=spaces[m]) for _, m in args],
        out_specs=[pl.BlockSpec(memory_space=spaces[m]) for _, m in outs],
        scratch_shapes=list(scratch),
        compiler_params=pltpu.CompilerParams(vmem_limit_bytes=limit),
    )(*arrays)


def rotated(x, axis, by):
    n = lax.axis_size(axis)
    return lax.ppermute(x, axis, [(i, (i + by) % n) for i in range(n)])


def traded(one, two):
    size = lax.axis_size("sub")
    groups = lax.axis_size("grp")
    outs = []
    for x, first in ((one, 0), (two, 1)):
        pairs = []
        for g in range(groups):
            for c in range(size):
                other = c + 1 if c % 2 == first else c - 1
                if 0 <= other < size:
                    pairs.append((g * size + c, g * size + other))
                else:
                    pairs.append((g * size + c, (g ^ 1) * size + c))
        outs.append(lax.ppermute(x, ("grp", "sub"), pairs))
    return outs


def body(fine_res, node_map, connect, grads, moduli, mass):
    size = lax.axis_size("sub")
    groups = lax.axis_size("grp")
    own = mass.shape[0]
    fine = node_map.shape[1]
    elems = connect.shape[1]
    rows = (own + CI) // LO
    k = CI // LO
    col = lax.axis_index("sub").astype(jnp.int32).reshape(1)
    fcount = 2 * fine // LANE
    ecount = 4 * elems // LANE

    def kept(*shape, dtype=jnp.float32):
        return pltpu.VMEM(shape, dtype), "v"

    table = kept(3 * HP, LO)
    edge = kept(3 * k, LO)
    acc = pltpu.VMEM((9 * HP, LO), jnp.float32)
    parts = pltpu.VMEM((9 * ecount, LANE), jnp.float32)
    strain = kept(6 * elems // LANE, LANE)
    mass2 = mass.reshape(own // LANE, LANE)

    partial, one, two, map_idx = call(
        functools.partial(rhs_kernel, own=own),
        [(col, "s"), (node_map, "h"), (fine_res, "h"), (mass2, "h")],
        [table, kept(4 * k, LO), kept(4 * k, LO), kept(fcount, LANE, dtype=jnp.int32)],
        [pltpu.VMEM((3 * fcount // 2, LANE), jnp.float32), pltpu.VMEM((LANE, fcount), jnp.int32),
         pltpu.VMEM((9 * fcount, LANE), jnp.float32), acc],
    )
    one, two = traded(one, two)
    idx, cols, g, mod = call(
        functools.partial(prep_kernel, own=own),
        [(col, "s"), (connect, "h"), (grads, "h"), (moduli, "h")],
        [kept(ecount, LANE, dtype=jnp.int32), kept(LANE, ecount, dtype=jnp.int32), kept(9 * elems // LANE, LANE), kept(2 * elems // LANE, LANE)],
    )
    part, mass_ext = call(
        functools.partial(halo_kernel, own=own, size=size),
        [(col, "s"), (partial, "v"), (one, "v"), (two, "v"), (mass2, "h"), (mod, "v")],
        [table, kept(HP, LO)],
    )
    sums = [part] + [rotated(part, "grp", i) for i in range(1, groups)]
    (hot,) = call(hot_kernel, [(cols, "v")], [kept(ecount * LANE, LO, dtype=jnp.bfloat16)], limit=ROOM)
    elements = [(idx, "v"), (g, "v"), (mod, "v")]
    summing = [(idx, "v"), (hot, "v"), (g, "v"), (mod, "v")]
    kw = dict(own=own, rows=rows)
    v0, f0, one, two, s0 = call(
        functools.partial(first_kernel, groups=groups, **kw),
        [(col, "s")] + [(x, "v") for x in sums] + summing,
        [table, table, edge, edge, strain],
        [parts],
        ROOM,
    )
    one, two = traded(one, two)
    v1, f1, one, two, s1 = call(
        functools.partial(second_kernel, size=size, **kw),
        [(col, "s"), (one, "v"), (two, "v"), (v0, "v"), (f0, "v"), (mass_ext, "v")] + summing,
        [table, table, edge, edge, strain],
        [parts],
        ROOM,
    )
    one, two = traded(one, two)
    msg, v2 = call(
        functools.partial(third_kernel, size=size, **kw),
        [(col, "s")] + [(x, "v") for x in (one, two, v0, v1, f1, s0, s1, mass_ext)] + elements,
        [kept(size, 8, LANE), table],
        [pltpu.VMEM((6 * elems // LANE, LANE), jnp.float32)],
    )
    recv = lax.all_to_all(msg, "sub", 0, 0)
    (out,) = call(
        functools.partial(last_kernel, rows=rows),
        [(recv, "v"), (v0, "v"), (v1, "v"), (v2, "v"), (map_idx, "v")],
        [(jax.ShapeDtypeStruct((3, fine), jnp.float32), "h")],
        [pltpu.VMEM((3 * HP, LO), jnp.float32)],
    )
    return out


def solution(mesh):
    in_specs = (
        P(None, ("grp", "sub")),
        P(None, ("grp", "sub")),
        P(None, "sub"),
        P(None, None, "sub"),
        P(None, "sub"),
        P("sub"),
    )
    out_specs = P(None, ("grp", "sub"))
    return jax.shard_map(body, mesh=mesh, in_specs=in_specs, out_specs=out_specs, check_vma=False)
```

```python
import functools

import jax
import jax.numpy as jnp
from jax import lax
from jax.experimental import pallas as pl
from jax.experimental.pallas import tpu as pltpu
from jax.sharding import PartitionSpec as P

CI = 1024
LANE = 128
LO = 256
HP = 16
ROOM = 16 << 20
RC = 32

PAIRS = ((0, 0), (1, 1), (2, 2), (0, 1), (0, 2), (1, 2))
SYM = ((0, 3, 4), (3, 1, 5), (4, 5, 2))


def split3(x):
    a = x.astype(jnp.bfloat16).astype(jnp.float32)
    r = x - a
    b = r.astype(jnp.bfloat16).astype(jnp.float32)
    return a, b, r - b


def gather(table, idxs, rows):
    out = []
    for ix in idxs:
        lo = ix & (LANE - 1)
        hi = ix >> 7
        got = [jnp.zeros((8, LANE), jnp.float32)] * 3
        for h in range(rows * LO // LANE):
            r, half = divmod(h, LO // LANE)
            mask = hi == h
            for c in range(3):
                row = table[c * HP + r : c * HP + r + 1, half * LANE : (half + 1) * LANE]
                row = jnp.broadcast_to(row, (8, LANE))
                moved = jnp.take_along_axis(row, lo, axis=1, mode="promise_in_bounds")
                got[c] = jnp.where(mask, moved, got[c])
        out.append(got)
    return out


def scatter(idx_ref, cols_ref, parts_ref, acc_ref, count):
    hi_iota = lax.broadcasted_iota(jnp.int32, (HP, LANE), 0)
    lo_iota = lax.broadcasted_iota(jnp.int32, (LANE, LO), 1).astype(jnp.float32).astype(jnp.bfloat16)
    one = jnp.bfloat16(1)
    zero = jnp.bfloat16(0)
    acc_ref[...] = jnp.zeros(acc_ref.shape, jnp.float32)
    for i in range(count // RC):
        hot, moved = [], []
        for row in range(i * RC, i * RC + RC):
            lo = (cols_ref[:, row : row + 1] & (LO - 1)).astype(jnp.float32)
            lo = jnp.broadcast_to(lo, (LANE, LANE)).astype(jnp.bfloat16)
            hot.append(jnp.where(lo_iota == jnp.concatenate([lo, lo], axis=1), one, zero))
            mask = hi_iota == (idx_ref[row : row + 1, :] >> 8)
            group = [
                jnp.where(mask, parts_ref[p * count + row : p * count + row + 1, :], 0.0).astype(jnp.bfloat16)
                for p in range(9)
            ]
            moved.append(jnp.concatenate(group, axis=0))
        acc_ref[...] += lax.dot_general(
            jnp.concatenate(moved, axis=1),
            jnp.concatenate(hot, axis=0),
            (((1,), (0,)), ((), ())),
            preferred_element_type=jnp.float32,
        )
    n = 3 * HP
    return acc_ref[:n] + acc_ref[n : 2 * n] + acc_ref[2 * n :]


def lines(ref, lead, dst, base, f=lambda x: x, group=8):
    n = ref.shape[-1] // LANE
    for q in range(n):
        to = base + q // 8 * group + q % 8
        dst[to : to + 1, :] = f(ref[lead + (slice(q * LANE, (q + 1) * LANE),)])


def rhs_kernel(col_ref, map_ref, fine_ref, mass_ref, out_ref, one_ref, two_ref, idx_ref, mine_ref,
               half_ref, cols_ref, parts_ref, acc_ref, *, own):
    half = map_ref.shape[1] // LANE
    count = 2 * half
    shift = col_ref[0] * own
    for k in range(2):
        lines(map_ref, (slice(k, k + 1),), idx_ref, k * half, lambda x: x - shift)
    cols_ref[...] = jnp.transpose(idx_ref[...])
    for c in range(3):
        lines(fine_ref, (slice(c, c + 1),), half_ref, c * half)
    for c in range(3):
        pieces = split3(0.5 * half_ref[c * half : (c + 1) * half, :])
        for s in range(3):
            for k in range(2):
                at = (s * 3 + c) * count + k * half
                parts_ref[at : at + half, :] = pieces[s]
    table = scatter(idx_ref, cols_ref, parts_ref, acc_ref, count)
    out_ref[...] = table
    k = CI // LO
    lower, upper = shared(table, own)
    mine = jnp.concatenate(
        [mass_ref[pl.ds(0, own // LO, stride=2), :], mass_ref[pl.ds(1, own // LO, stride=2), :]], axis=1
    )
    mine_ref[...] = mine
    mass = mine[:k]
    send(one_ref, two_ref, col_ref[0], jnp.concatenate([lower, mass], axis=0), jnp.concatenate([upper, mass], axis=0))


def prep_kernel(col_ref, conn_ref, grads_ref, moduli_ref, idx_ref, cols_ref, g_ref, m_ref, *, own):
    per = moduli_ref.shape[1] // LANE
    shift = col_ref[0] * own
    for a in range(4):
        lines(conn_ref, (slice(a, a + 1),), idx_ref, a * 8, lambda x: x - shift, 32)
    cols_ref[...] = jnp.transpose(idx_ref[...])
    for d in range(3):
        for a in range(3):
            lines(grads_ref, (d, slice(a, a + 1)), g_ref, (d * 3 + a) * per)
    for i in range(2):
        lines(moduli_ref, (slice(i, i + 1),), m_ref, i * per)


def hot_kernel(cols_ref, hot_ref):
    lo_iota = lax.broadcasted_iota(jnp.int32, (LANE, LO), 1).astype(jnp.float32).astype(jnp.bfloat16)
    for row in range(cols_ref.shape[1]):
        lo = (cols_ref[:, row : row + 1] & (LO - 1)).astype(jnp.float32)
        lo = jnp.broadcast_to(lo, (LANE, LANE)).astype(jnp.bfloat16)
        hit = lo_iota == jnp.concatenate([lo, lo], axis=1)
        hot_ref[row * LANE : (row + 1) * LANE, :] = jnp.where(hit, jnp.bfloat16(1), jnp.bfloat16(0))


def shared(table, own):
    k = CI // LO
    base = own // LO
    lower = jnp.concatenate([table[c * HP : c * HP + k] for c in range(3)], axis=0)
    upper = jnp.concatenate([table[c * HP + base : c * HP + base + k] for c in range(3)], axis=0)
    return lower, upper


def send(one_ref, two_ref, col, lower, upper):
    even = col % 2 == 0
    one_ref[...] = jnp.where(even, upper, lower)
    two_ref[...] = jnp.where(even, lower, upper)


def received(one_ref, two_ref, col):
    even = col % 2 == 0
    one, two = one_ref[...], two_ref[...]
    return jnp.where(even, two, one), jnp.where(even, one, two)


def halo_kernel(col_ref, table_ref, one_ref, two_ref, mine_ref, moduli_ref, out_ref, mass_out_ref, *, own, size):
    col = col_ref[0]
    k = CI // LO
    before, after = received(one_ref, two_ref, col)
    out_ref[...] = add_halo(table_ref[...], col, before[: 3 * k], after[: 3 * k], own, size)
    pad = jnp.zeros((HP - own // LO - k, LO), jnp.float32)
    mass_out_ref[...] = jnp.concatenate([mine_ref[...], after[3 * k :], pad], axis=0)


def element_strains(table, idx_ref, grads_ref, strain_ref, j, rows):
    per = grads_ref.shape[0] // 9
    at = j * 8
    v = gather(table, [idx_ref[j * 32 + k * 8 : j * 32 + k * 8 + 8, :] for k in range(4)], rows)
    g = [[grads_ref[(d * 3 + a) * per + at : (d * 3 + a) * per + at + 8, :] for d in range(3)] for a in range(3)]
    w = [[v[a][i] - v[3][i] for i in range(3)] for a in range(3)]
    grad = [[w[0][i] * g[0][j] + w[1][i] * g[1][j] + w[2][i] * g[2][j] for j in range(3)] for i in range(3)]
    strain = [0.5 * (grad[i][j] + grad[j][i]) for i, j in PAIRS]
    for p in range(6):
        strain_ref[p * per + at : p * per + at + 8, :] = strain[p]
    return strain, g


def apply_elements(col, table, idx_ref, hot_ref, grads_ref, moduli_ref, strain_ref, parts_ref, acc_ref, rows):
    per = moduli_ref.shape[0] // 2
    count = 4 * per
    hi_iota = lax.broadcasted_iota(jnp.int32, (HP, LANE), 0)
    acc_ref[...] = jnp.zeros((9 * HP, LO), jnp.float32)

    def forces(j):
        at = j * 8
        strain, g = element_strains(table, idx_ref, grads_ref, strain_ref, j, rows)
        stress = stresses(strain, moduli_ref[at : at + 8, :], moduli_ref[per + at : per + at + 8, :])
        for i in range(3):
            f = [sum(stress[SYM[i][j]] * g[a][j] for j in range(3)) for a in range(3)]
            f.append(-(f[0] + f[1] + f[2]))
            for a in range(4):
                pieces = split3(f[a])
                for s in range(3):
                    to = (s * 3 + i) * count + j * 32 + a * 8
                    parts_ref[to : to + 8, :] = pieces[s]

    def summed(j):
        moved = []
        for row in range(j * 32, j * 32 + 32):
            mask = hi_iota == (idx_ref[row : row + 1, :] >> 8)
            group = [
                jnp.where(mask, parts_ref[p * count + row : p * count + row + 1, :], 0.0).astype(jnp.bfloat16)
                for p in range(9)
            ]
            moved.append(jnp.concatenate(group, axis=0))
        acc_ref[...] += jnp.dot(
            jnp.concatenate(moved, axis=1),
            hot_ref[j * 32 * LANE : (j + 1) * 32 * LANE, :],
            preferred_element_type=jnp.float32,
        )

    for j in range(per // 8 + 1):

        @pl.when(col >= 0)
        def _():
            if j > 0:
                summed(j - 1)
            if j < per // 8:
                forces(j)

    n = 3 * HP
    return acc_ref[:n] + acc_ref[n : 2 * n] + acc_ref[2 * n :]


def stresses(strain, lam, mu):
    bulk = lam * (strain[0] + strain[1] + strain[2])
    return [2.0 * mu * strain[p] + (bulk if p < 3 else 0.0) for p in range(6)]


def work(stress, strain):
    diag = stress[0] * strain[0] + stress[1] * strain[1] + stress[2] * strain[2]
    return diag + 2.0 * (stress[3] * strain[3] + stress[4] * strain[4] + stress[5] * strain[5])


def own_rows(own):
    r = lax.broadcasted_iota(jnp.int32, (3 * HP, LO), 0) & (HP - 1)
    return r < own // LO


def per_component(x):
    return jnp.concatenate([x, x, x], axis=0)


def add_halo(own_part, col, down, up, own, size):
    k = CI // LO
    down = jnp.where(col > 0, down, 0.0)
    up = jnp.where(col < size - 1, up, 0.0)
    pieces = []
    for c in range(3):
        pieces.append(down[c * k : (c + 1) * k])
        pieces.append(jnp.zeros((own // LO - k, LO), jnp.float32))
        pieces.append(up[c * k : (c + 1) * k])
        pieces.append(jnp.zeros((HP - own // LO - k, LO), jnp.float32))
    return own_part + jnp.concatenate(pieces, axis=0)


def first_kernel(col_ref, *refs, own, rows, groups):
    sum_refs = refs[:groups]
    (idx_ref, hot_ref, grads_ref, moduli_ref, v_ref, f_ref, one_ref, two_ref, strain_ref, parts_ref,
     acc_ref) = refs[groups:]
    total = sum_refs[0][...]
    for ref in sum_refs[1:]:
        total = total + ref[...]
    v_ref[...] = total
    f = apply_elements(col_ref[0], v_ref, idx_ref, hot_ref, grads_ref, moduli_ref, strain_ref, parts_ref, acc_ref, rows)
    f_ref[...] = f
    send(one_ref, two_ref, col_ref[0], *shared(f, own))


def second_kernel(col_ref, one_ref, two_ref, v0_ref, f0_ref, mass_ref, idx_ref, hot_ref, grads_ref, moduli_ref,
                  v_ref, f_ref, one_out_ref, two_out_ref, strain_ref, parts_ref, acc_ref, *, own, rows, size):
    mass = per_component(mass_ref[...])
    before, after = received(one_ref, two_ref, col_ref[0])
    v_ref[...] = add_halo(f0_ref[...] + mass * v0_ref[...], col_ref[0], before, after, own, size)
    f = apply_elements(col_ref[0], v_ref, idx_ref, hot_ref, grads_ref, moduli_ref, strain_ref, parts_ref, acc_ref, rows)
    f_ref[...] = f
    send(one_out_ref, two_out_ref, col_ref[0], *shared(f, own))


def total(x):
    return jnp.sum(x, axis=(0, 1), keepdims=True)


def ratio(a, b):
    return jnp.where(b > 0.0, a / jnp.where(b > 0.0, b, 1.0), 0.0)


def third_kernel(col_ref, one_ref, two_ref, v0_ref, v1_ref, f1_ref, s0_ref, s1_ref, mass_ref, idx_ref,
                 grads_ref, moduli_ref, msg_ref, v2_ref, s2_ref, *, own, rows, size):
    mass = per_component(mass_ref[...])
    before, after = received(one_ref, two_ref, col_ref[0])
    v2 = add_halo(f1_ref[...] + mass * v1_ref[...], col_ref[0], before, after, own, size)
    v2_ref[...] = v2
    mine = own_rows(own)
    x0 = jnp.where(mine, v0_ref[...], 0.0)
    x1 = jnp.where(mine, v1_ref[...], 0.0)
    x2 = jnp.where(mine, v2, 0.0)
    rr0 = total(x0 * x0)
    n1 = total(x1 * x1)
    usable = (rr0 > 0.0) & (n1 > 0.0)
    s = jnp.where(usable, jnp.sqrt(jnp.where(usable, rr0, 1.0)) / jnp.sqrt(jnp.where(usable, n1, 1.0)), 1.0)
    v = s * x1
    z = s * (s * x2)
    vv = total(v * v)
    a = ratio(total(x0 * v), vv)
    q = ratio(total(z * v), vv)
    u = x0 - a * v
    w = z - q * v
    t = v - a * z
    uw = total(u * w)
    ww = total(w * w)
    g = ratio(uw, ww)
    b = u - g * w
    dots = [s, a, q, g, rr0, total(u * u), total(u * v), vv, total(u * t), uw, total(v * t), total(v * w),
            total(b * b), total(b * v), total(b * w), ww, total(b * t), total(w * t)]
    weight = jnp.where(mine, mass, 0.0)
    pairs = [(b, b), (b, v), (b, w), (v, v), (v, w), (w, w)]
    energy = [total(weight * (l * r)) for l, r in pairs]

    per = moduli_ref.shape[0] // 2
    for j in range(per // 8):
        element_strains(v2_ref, idx_ref, grads_ref, s2_ref, j, rows)

    def step(j, sums):
        at = j * 8
        lam = moduli_ref[at : at + 8, :]
        mu = moduli_ref[per + at : per + at + 8, :]
        e0, e1, e2 = [[ref[p * per + at : p * per + at + 8, :] for p in range(6)] for ref in (s0_ref, s1_ref, s2_ref)]
        ev = [s * e for e in e1]
        ew = [s * (s * e) - q * h for e, h in zip(e2, ev)]
        eb = [e - a * h - g * k for e, h, k in zip(e0, ev, ew)]
        tb, tv, tw = [stresses(e, lam, mu) for e in (eb, ev, ew)]
        new = [work(tb, eb), work(tb, ev), work(tb, ew), work(tv, ev), work(tv, ew), work(tw, ew)]
        return tuple(x + y for x, y in zip(sums, new))

    sums = (jnp.zeros((8, LANE), jnp.float32),) * 6
    for j in range(per // 8):
        sums = step(j, sums)
    numbers = dots + [e + total(x) for e, x in zip(energy, sums)]
    lane = lax.broadcasted_iota(jnp.int32, (1, LANE), 1)
    lines_ = []
    for r in range(8):
        line = jnp.broadcast_to(numbers[r], (1, LANE))
        for i in range(r + 8, len(numbers), 8):
            line = jnp.where(lane < i // 8 * (LANE // 4), line, numbers[i])
        lines_.append(line)
    msg_ref[...] = jnp.broadcast_to(jnp.concatenate(lines_, axis=0)[None], msg_ref.shape)


def last_kernel(recv_ref, v0_ref, v1_ref, v2_ref, idx_ref, out_ref, table_ref, *, rows):
    size = recv_ref.shape[0]

    def number(i):
        at = i // 8 * (LANE // 4)
        return jnp.broadcast_to(recv_ref[:, i % 8, :][:, at : at + 1], (size, LANE))

    def over(x):
        return jnp.sum(x, axis=0, keepdims=True)

    (s, a, q, g, rr0, uu, uv, vv, ut, uw, vt, vw, bb, bv, bw, ww, bt, wt,
     ebb, ebv, ebw, evv, evw, eww) = [number(i) for i in range(24)]
    inv = 1.0 / s
    rr0 = over(rr0)
    curv0 = over(inv * (uv + a * vv))
    alpha0 = rr0 / curv0
    a0 = alpha0 * inv
    d = a - a0
    rr1 = over(uu + d * (2.0 * uv + d * vv))
    own1 = over(inv * (ut + d * (uw + q * uv + vt + d * (vw + q * vv))))
    cross1 = over(inv * (uv + d * vv))
    beta0 = rr1 / rr0
    curv1 = own1 + beta0 * (2.0 * cross1 + beta0 * curv0)
    alpha1 = rr1 / curv1
    a1 = alpha1 * inv
    c2 = a0 * a1
    m1 = g + c2
    m0 = a - a0 - a1 * (1.0 + beta0) + q * c2
    h = d * q + beta0
    rr2 = over(bb + m0 * (2.0 * bv + m0 * vv) + m1 * (2.0 * (bw + m0 * vw) + m1 * ww))
    cross2 = over(inv * (bt + d * bw + h * bv + m0 * (vt + d * vw + h * vv) + m1 * (wt + d * ww + h * vw)))
    own2 = over(ebb + m0 * (2.0 * ebv + m0 * evv) + m1 * (2.0 * (ebw + m0 * evw) + m1 * eww))
    beta1 = rr2 / rr1
    curv2 = own2 + beta1 * (2.0 * cross2 + beta1 * curv1)
    alpha2 = rr2 / curv2

    wide = lambda x: jnp.concatenate([x, x], axis=1)
    alpha0, alpha1, alpha2, beta0, beta1 = [wide(x) for x in (alpha0, alpha1, alpha2, beta0, beta1)]
    v0 = v0_ref[...]
    v1 = v1_ref[...]
    r1 = v0 - alpha0 * v1
    d1 = r1 + beta0 * v0
    image1 = (v1 - alpha0 * v2_ref[...]) + beta0 * v1
    r2 = r1 - alpha1 * image1
    d2 = r2 + beta1 * d1
    table_ref[...] = 0.5 * (alpha0 * v0 + alpha1 * d1 + alpha2 * d2)
    per = idx_ref.shape[0] // 2
    for j in range(per // 8):
        v = gather(table_ref, [idx_ref[k * per + j * 8 : k * per + j * 8 + 8, :] for k in range(2)], rows)
        for c in range(3):
            got = v[0][c] + v[1][c]
            for q in range(8):
                at = (j * 8 + q) * LANE
                out_ref[c : c + 1, at : at + LANE] = got[q : q + 1, :]


def call(kernel, args, outs, scratch=(), limit=None):
    spaces = {"s": pltpu.SMEM, "v": pltpu.VMEM, "h": pltpu.VMEM}
    arrays = [pltpu.with_memory_space_constraint(x, pltpu.VMEM) if m == "v" else x for x, m in args]
    return pl.pallas_call(
        kernel,
        out_shape=[o for o, _ in outs],
        in_specs=[pl.BlockSpec(memory_space=spaces[m]) for _, m in args],
        out_specs=[pl.BlockSpec(memory_space=spaces[m]) for _, m in outs],
        scratch_shapes=list(scratch),
        compiler_params=pltpu.CompilerParams(vmem_limit_bytes=limit),
    )(*arrays)


def rotated(x, axis, by):
    n = lax.axis_size(axis)
    return lax.ppermute(x, axis, [(i, (i + by) % n) for i in range(n)])


def traded(one, two):
    size = lax.axis_size("sub")
    groups = lax.axis_size("grp")
    outs = []
    for x, first in ((one, 0), (two, 1)):
        pairs = []
        for g in range(groups):
            for c in range(size):
                other = c + 1 if c % 2 == first else c - 1
                if 0 <= other < size:
                    pairs.append((g * size + c, g * size + other))
                else:
                    pairs.append((g * size + c, (g ^ 1) * size + c))
        outs.append(lax.ppermute(x, ("grp", "sub"), pairs))
    return outs


def body(fine_res, node_map, connect, grads, moduli, mass):
    size = lax.axis_size("sub")
    groups = lax.axis_size("grp")
    own = mass.shape[0]
    fine = node_map.shape[1]
    elems = connect.shape[1]
    rows = (own + CI) // LO
    k = CI // LO
    col = lax.axis_index("sub").astype(jnp.int32).reshape(1)
    fcount = 2 * fine // LANE
    ecount = 4 * elems // LANE

    def kept(*shape, dtype=jnp.float32):
        return pltpu.VMEM(shape, dtype), "v"

    table = kept(3 * HP, LO)
    edge = kept(3 * k, LO)
    acc = pltpu.VMEM((9 * HP, LO), jnp.float32)
    parts = pltpu.VMEM((9 * ecount, LANE), jnp.float32)
    strain = kept(6 * elems // LANE, LANE)
    mass2 = mass.reshape(own // LANE, LANE)

    partial, one, two, map_idx, mine = call(
        functools.partial(rhs_kernel, own=own),
        [(col, "s"), (node_map, "h"), (fine_res, "h"), (mass2, "h")],
        [table, kept(4 * k, LO), kept(4 * k, LO), kept(fcount, LANE, dtype=jnp.int32), kept(own // LO, LO)],
        [pltpu.VMEM((3 * fcount // 2, LANE), jnp.float32), pltpu.VMEM((LANE, fcount), jnp.int32),
         pltpu.VMEM((9 * fcount, LANE), jnp.float32), acc],
    )
    one, two = traded(one, two)
    idx, cols, g, mod = call(
        functools.partial(prep_kernel, own=own),
        [(col, "s"), (connect, "h"), (grads, "h"), (moduli, "h")],
        [kept(ecount, LANE, dtype=jnp.int32), kept(LANE, ecount, dtype=jnp.int32), kept(9 * elems // LANE, LANE), kept(2 * elems // LANE, LANE)],
    )
    part, mass_ext = call(
        functools.partial(halo_kernel, own=own, size=size),
        [(col, "s"), (partial, "v"), (one, "v"), (two, "v"), (mine, "v"), (mod, "v")],
        [table, kept(HP, LO)],
    )
    sums = [part] + [rotated(part, "grp", i) for i in range(1, groups)]
    (hot,) = call(hot_kernel, [(cols, "v")], [kept(ecount * LANE, LO, dtype=jnp.bfloat16)], limit=ROOM)
    elements = [(idx, "v"), (g, "v"), (mod, "v")]
    summing = [(idx, "v"), (hot, "v"), (g, "v"), (mod, "v")]
    kw = dict(own=own, rows=rows)
    v0, f0, one, two, s0 = call(
        functools.partial(first_kernel, groups=groups, **kw),
        [(col, "s")] + [(x, "v") for x in sums] + summing,
        [table, table, edge, edge, strain],
        [parts, acc],
        ROOM,
    )
    one, two = traded(one, two)
    v1, f1, one, two, s1 = call(
        functools.partial(second_kernel, size=size, **kw),
        [(col, "s"), (one, "v"), (two, "v"), (v0, "v"), (f0, "v"), (mass_ext, "v")] + summing,
        [table, table, edge, edge, strain],
        [parts, acc],
        ROOM,
    )
    one, two = traded(one, two)
    msg, v2 = call(
        functools.partial(third_kernel, size=size, **kw),
        [(col, "s")] + [(x, "v") for x in (one, two, v0, v1, f1, s0, s1, mass_ext)] + elements,
        [kept(size, 8, LANE), table],
        [pltpu.VMEM((6 * elems // LANE, LANE), jnp.float32)],
    )
    recv = lax.all_to_all(msg, "sub", 0, 0)
    (out,) = call(
        functools.partial(last_kernel, rows=rows),
        [(recv, "v"), (v0, "v"), (v1, "v"), (v2, "v"), (map_idx, "v")],
        [(jax.ShapeDtypeStruct((3, fine), jnp.float32), "h")],
        [pltpu.VMEM((3 * HP, LO), jnp.float32)],
    )
    return out


def solution(mesh):
    in_specs = (
        P(None, ("grp", "sub")),
        P(None, ("grp", "sub")),
        P(None, "sub"),
        P(None, None, "sub"),
        P(None, "sub"),
        P("sub"),
    )
    out_specs = P(None, ("grp", "sub"))
    return jax.shard_map(body, mesh=mesh, in_specs=in_specs, out_specs=out_specs, check_vma=False)
```

```python
import functools

import jax
import jax.numpy as jnp
from jax import lax
from jax.experimental import pallas as pl
from jax.experimental.pallas import tpu as pltpu
from jax.sharding import PartitionSpec as P

CI = 1024
LANE = 128
LO = 256
HP = 16
ROOM = 16 << 20
RC = 32

PAIRS = ((0, 0), (1, 1), (2, 2), (0, 1), (0, 2), (1, 2))
SYM = ((0, 3, 4), (3, 1, 5), (4, 5, 2))


def split3(x):
    a = x.astype(jnp.bfloat16).astype(jnp.float32)
    r = x - a
    b = r.astype(jnp.bfloat16).astype(jnp.float32)
    return a, b, r - b


def gather(table, idxs, rows):
    out = []
    for ix in idxs:
        lo = ix & (LANE - 1)
        hi = ix >> 7
        got = [jnp.zeros((8, LANE), jnp.float32)] * 3
        for h in range(rows * LO // LANE):
            r, half = divmod(h, LO // LANE)
            mask = hi == h
            for c in range(3):
                row = table[c * HP + r : c * HP + r + 1, half * LANE : (half + 1) * LANE]
                row = jnp.broadcast_to(row, (8, LANE))
                moved = jnp.take_along_axis(row, lo, axis=1, mode="promise_in_bounds")
                got[c] = jnp.where(mask, moved, got[c])
        out.append(got)
    return out


def scatter(idx_ref, cols_ref, parts_ref, acc_ref, count):
    hi_iota = lax.broadcasted_iota(jnp.int32, (HP, LANE), 0)
    lo_iota = lax.broadcasted_iota(jnp.int32, (LANE, LO), 1).astype(jnp.float32).astype(jnp.bfloat16)
    one = jnp.bfloat16(1)
    zero = jnp.bfloat16(0)
    acc_ref[...] = jnp.zeros(acc_ref.shape, jnp.float32)
    for i in range(count // RC):
        hot, moved = [], []
        for row in range(i * RC, i * RC + RC):
            lo = jnp.broadcast_to(cols_ref[:, row : row + 1], (LANE, LANE)).astype(jnp.bfloat16)
            hot.append(jnp.where(lo_iota == jnp.concatenate([lo, lo], axis=1), one, zero))
            mask = hi_iota == (idx_ref[row : row + 1, :] >> 8)
            group = [
                jnp.where(mask, parts_ref[p * count + row : p * count + row + 1, :], 0.0).astype(jnp.bfloat16)
                for p in range(9)
            ]
            moved.append(jnp.concatenate(group, axis=0))
        acc_ref[...] += lax.dot_general(
            jnp.concatenate(moved, axis=1),
            jnp.concatenate(hot, axis=0),
            (((1,), (0,)), ((), ())),
            preferred_element_type=jnp.float32,
        )
    n = 3 * HP
    return acc_ref[:n] + acc_ref[n : 2 * n] + acc_ref[2 * n :]


def lines(ref, lead, dst, base, f=lambda x: x, group=8):
    n = ref.shape[-1] // LANE
    for q in range(n):
        to = base + q // 8 * group + q % 8
        dst[to : to + 1, :] = f(ref[lead + (slice(q * LANE, (q + 1) * LANE),)])


def rhs_kernel(col_ref, map_ref, fine_ref, mass_ref, out_ref, one_ref, two_ref, idx_ref, mine_ref,
               half_ref, cols_ref, parts_ref, acc_ref, *, own):
    half = map_ref.shape[1] // LANE
    count = 2 * half
    shift = col_ref[0] * own
    for k in range(2):
        lines(map_ref, (slice(k, k + 1),), idx_ref, k * half, lambda x: x - shift)
    cols_ref[...] = jnp.transpose((idx_ref[...] & (LO - 1)).astype(jnp.float32))
    for c in range(3):
        lines(fine_ref, (slice(c, c + 1),), half_ref, c * half)
    for c in range(3):
        pieces = split3(0.5 * half_ref[c * half : (c + 1) * half, :])
        for s in range(3):
            for k in range(2):
                at = (s * 3 + c) * count + k * half
                parts_ref[at : at + half, :] = pieces[s]
    table = scatter(idx_ref, cols_ref, parts_ref, acc_ref, count)
    out_ref[...] = table
    k = CI // LO
    lower, upper = shared(table, own)
    mine = jnp.concatenate(
        [mass_ref[pl.ds(0, own // LO, stride=2), :], mass_ref[pl.ds(1, own // LO, stride=2), :]], axis=1
    )
    mine_ref[...] = mine
    mass = mine[:k]
    send(one_ref, two_ref, col_ref[0], jnp.concatenate([lower, mass], axis=0), jnp.concatenate([upper, mass], axis=0))


def prep_kernel(col_ref, conn_ref, grads_ref, moduli_ref, idx_ref, cols_ref, g_ref, m_ref, *, own):
    per = moduli_ref.shape[1] // LANE
    shift = col_ref[0] * own
    for a in range(4):
        lines(conn_ref, (slice(a, a + 1),), idx_ref, a * 8, lambda x: x - shift, 32)
    cols_ref[...] = jnp.transpose((idx_ref[...] & (LO - 1)).astype(jnp.float32))
    for d in range(3):
        for a in range(3):
            lines(grads_ref, (d, slice(a, a + 1)), g_ref, (d * 3 + a) * per)
    for i in range(2):
        lines(moduli_ref, (slice(i, i + 1),), m_ref, i * per)


def hot_kernel(cols_ref, hot_ref):
    lo_iota = lax.broadcasted_iota(jnp.int32, (LANE, LO), 1).astype(jnp.float32).astype(jnp.bfloat16)
    for row in range(cols_ref.shape[1]):
        lo = jnp.broadcast_to(cols_ref[:, row : row + 1], (LANE, LANE)).astype(jnp.bfloat16)
        hit = lo_iota == jnp.concatenate([lo, lo], axis=1)
        hot_ref[row * LANE : (row + 1) * LANE, :] = jnp.where(hit, jnp.bfloat16(1), jnp.bfloat16(0))


def shared(table, own):
    k = CI // LO
    base = own // LO
    lower = jnp.concatenate([table[c * HP : c * HP + k] for c in range(3)], axis=0)
    upper = jnp.concatenate([table[c * HP + base : c * HP + base + k] for c in range(3)], axis=0)
    return lower, upper


def send(one_ref, two_ref, col, lower, upper):
    even = col % 2 == 0
    one_ref[...] = jnp.where(even, upper, lower)
    two_ref[...] = jnp.where(even, lower, upper)


def received(one_ref, two_ref, col):
    even = col % 2 == 0
    one, two = one_ref[...], two_ref[...]
    return jnp.where(even, two, one), jnp.where(even, one, two)


def halo_kernel(col_ref, table_ref, one_ref, two_ref, mine_ref, moduli_ref, out_ref, mass_out_ref, *, own, size):
    col = col_ref[0]
    k = CI // LO
    before, after = received(one_ref, two_ref, col)
    out_ref[...] = add_halo(table_ref[...], col, before[: 3 * k], after[: 3 * k], own, size)
    pad = jnp.zeros((HP - own // LO - k, LO), jnp.float32)
    mass_out_ref[...] = jnp.concatenate([mine_ref[...], after[3 * k :], pad], axis=0)


def element_strains(table, idx_ref, grads_ref, strain_ref, j, rows):
    per = grads_ref.shape[0] // 9
    at = j * 8
    v = gather(table, [idx_ref[j * 32 + k * 8 : j * 32 + k * 8 + 8, :] for k in range(4)], rows)
    g = [[grads_ref[(d * 3 + a) * per + at : (d * 3 + a) * per + at + 8, :] for d in range(3)] for a in range(3)]
    w = [[v[a][i] - v[3][i] for i in range(3)] for a in range(3)]
    grad = [[w[0][i] * g[0][j] + w[1][i] * g[1][j] + w[2][i] * g[2][j] for j in range(3)] for i in range(3)]
    strain = [0.5 * (grad[i][j] + grad[j][i]) for i, j in PAIRS]
    for p in range(6):
        strain_ref[p * per + at : p * per + at + 8, :] = strain[p]
    return strain, g


def apply_elements(col, table, idx_ref, hot_ref, grads_ref, moduli_ref, strain_ref, parts_ref, acc_ref, rows):
    per = moduli_ref.shape[0] // 2
    count = 4 * per
    hi_iota = lax.broadcasted_iota(jnp.int32, (HP, LANE), 0)
    acc_ref[...] = jnp.zeros(acc_ref.shape, jnp.float32)

    def forces(j):
        at = j * 8
        strain, g = element_strains(table, idx_ref, grads_ref, strain_ref, j, rows)
        stress = stresses(strain, moduli_ref[at : at + 8, :], moduli_ref[per + at : per + at + 8, :])
        for i in range(3):
            f = [sum(stress[SYM[i][j]] * g[a][j] for j in range(3)) for a in range(3)]
            f.append(-(f[0] + f[1] + f[2]))
            for a in range(4):
                pieces = split3(f[a])
                for s in range(3):
                    to = (s * 3 + i) * count + j * 32 + a * 8
                    parts_ref[to : to + 8, :] = pieces[s]

    def summed(j):
        moved = []
        for row in range(j * 32, j * 32 + 32):
            mask = hi_iota == (idx_ref[row : row + 1, :] >> 8)
            group = [
                jnp.where(mask, parts_ref[p * count + row : p * count + row + 1, :], 0.0).astype(jnp.bfloat16)
                for p in range(9)
            ]
            moved.append(jnp.concatenate(group, axis=0))
        half = 16
        n = 9 * HP
        for h in range(2):
            at = (j * 32 + h * half) * LANE
            acc_ref[h * n : (h + 1) * n, :] += jnp.dot(
                jnp.concatenate(moved[h * half : (h + 1) * half], axis=1),
                hot_ref[at : at + half * LANE, :],
                preferred_element_type=jnp.float32,
            )

    for j in range(per // 8 + 1):

        @pl.when(col >= 0)
        def _():
            if j > 0:
                summed(j - 1)
            if j < per // 8:
                forces(j)

    n = 3 * HP
    return sum(acc_ref[p * n : (p + 1) * n] for p in range(6))


def stresses(strain, lam, mu):
    bulk = lam * (strain[0] + strain[1] + strain[2])
    return [2.0 * mu * strain[p] + (bulk if p < 3 else 0.0) for p in range(6)]


def work(stress, strain):
    diag = stress[0] * strain[0] + stress[1] * strain[1] + stress[2] * strain[2]
    return diag + 2.0 * (stress[3] * strain[3] + stress[4] * strain[4] + stress[5] * strain[5])


def own_rows(own):
    r = lax.broadcasted_iota(jnp.int32, (3 * HP, LO), 0) & (HP - 1)
    return r < own // LO


def per_component(x):
    return jnp.concatenate([x, x, x], axis=0)


def add_halo(own_part, col, down, up, own, size):
    k = CI // LO
    down = jnp.where(col > 0, down, 0.0)
    up = jnp.where(col < size - 1, up, 0.0)
    pieces = []
    for c in range(3):
        pieces.append(down[c * k : (c + 1) * k])
        pieces.append(jnp.zeros((own // LO - k, LO), jnp.float32))
        pieces.append(up[c * k : (c + 1) * k])
        pieces.append(jnp.zeros((HP - own // LO - k, LO), jnp.float32))
    return own_part + jnp.concatenate(pieces, axis=0)


def first_kernel(col_ref, *refs, own, rows, groups):
    sum_refs = refs[:groups]
    (idx_ref, hot_ref, grads_ref, moduli_ref, v_ref, f_ref, one_ref, two_ref, strain_ref, parts_ref,
     acc_ref) = refs[groups:]
    total = sum_refs[0][...]
    for ref in sum_refs[1:]:
        total = total + ref[...]
    v_ref[...] = total
    f = apply_elements(col_ref[0], v_ref, idx_ref, hot_ref, grads_ref, moduli_ref, strain_ref, parts_ref, acc_ref, rows)
    f_ref[...] = f
    send(one_ref, two_ref, col_ref[0], *shared(f, own))


def second_kernel(col_ref, one_ref, two_ref, v0_ref, f0_ref, mass_ref, idx_ref, hot_ref, grads_ref, moduli_ref,
                  v_ref, f_ref, one_out_ref, two_out_ref, strain_ref, parts_ref, acc_ref, *, own, rows, size):
    mass = per_component(mass_ref[...])
    before, after = received(one_ref, two_ref, col_ref[0])
    v_ref[...] = add_halo(f0_ref[...] + mass * v0_ref[...], col_ref[0], before, after, own, size)
    f = apply_elements(col_ref[0], v_ref, idx_ref, hot_ref, grads_ref, moduli_ref, strain_ref, parts_ref, acc_ref, rows)
    f_ref[...] = f
    send(one_out_ref, two_out_ref, col_ref[0], *shared(f, own))


def total(x):
    return jnp.sum(x, axis=(0, 1), keepdims=True)


def ratio(a, b):
    return jnp.where(b > 0.0, a / jnp.where(b > 0.0, b, 1.0), 0.0)


def third_kernel(col_ref, one_ref, two_ref, v0_ref, v1_ref, f1_ref, s0_ref, s1_ref, mass_ref, idx_ref,
                 grads_ref, moduli_ref, msg_ref, v2_ref, s2_ref, *, own, rows, size):
    mass = per_component(mass_ref[...])
    before, after = received(one_ref, two_ref, col_ref[0])
    v2 = add_halo(f1_ref[...] + mass * v1_ref[...], col_ref[0], before, after, own, size)
    v2_ref[...] = v2
    mine = own_rows(own)
    x0 = jnp.where(mine, v0_ref[...], 0.0)
    x1 = jnp.where(mine, v1_ref[...], 0.0)
    x2 = jnp.where(mine, v2, 0.0)
    rr0 = total(x0 * x0)
    n1 = total(x1 * x1)
    usable = (rr0 > 0.0) & (n1 > 0.0)
    s = jnp.where(usable, jnp.sqrt(jnp.where(usable, rr0, 1.0)) / jnp.sqrt(jnp.where(usable, n1, 1.0)), 1.0)
    v = s * x1
    z = s * (s * x2)
    vv = total(v * v)
    a = ratio(total(x0 * v), vv)
    q = ratio(total(z * v), vv)
    u = x0 - a * v
    w = z - q * v
    t = v - a * z
    uw = total(u * w)
    ww = total(w * w)
    g = ratio(uw, ww)
    b = u - g * w
    dots = [s, a, q, g, rr0, total(u * u), total(u * v), vv, total(u * t), uw, total(v * t), total(v * w),
            total(b * b), total(b * v), total(b * w), ww, total(b * t), total(w * t)]
    weight = jnp.where(mine, mass, 0.0)
    pairs = [(b, b), (b, v), (b, w), (v, v), (v, w), (w, w)]
    energy = [total(weight * (l * r)) for l, r in pairs]

    per = moduli_ref.shape[0] // 2
    for j in range(per // 8):
        element_strains(v2_ref, idx_ref, grads_ref, s2_ref, j, rows)

    def step(j, sums):
        at = j * 8
        lam = moduli_ref[at : at + 8, :]
        mu = moduli_ref[per + at : per + at + 8, :]
        e0, e1, e2 = [[ref[p * per + at : p * per + at + 8, :] for p in range(6)] for ref in (s0_ref, s1_ref, s2_ref)]
        ev = [s * e for e in e1]
        ew = [s * (s * e) - q * h for e, h in zip(e2, ev)]
        eb = [e - a * h - g * k for e, h, k in zip(e0, ev, ew)]
        tb, tv, tw = [stresses(e, lam, mu) for e in (eb, ev, ew)]
        new = [work(tb, eb), work(tb, ev), work(tb, ew), work(tv, ev), work(tv, ew), work(tw, ew)]
        return tuple(x + y for x, y in zip(sums, new))

    sums = (jnp.zeros((8, LANE), jnp.float32),) * 6
    for j in range(per // 8):
        sums = step(j, sums)
    numbers = dots + [e + total(x) for e, x in zip(energy, sums)]
    lane = lax.broadcasted_iota(jnp.int32, (1, LANE), 1)
    lines_ = []
    for r in range(8):
        line = jnp.broadcast_to(numbers[r], (1, LANE))
        for i in range(r + 8, len(numbers), 8):
            line = jnp.where(lane < i // 8 * (LANE // 4), line, numbers[i])
        lines_.append(line)
    msg_ref[...] = jnp.broadcast_to(jnp.concatenate(lines_, axis=0)[None], msg_ref.shape)


def last_kernel(recv_ref, v0_ref, v1_ref, v2_ref, idx_ref, out_ref, table_ref, *, rows):
    size = recv_ref.shape[0]

    def number(i):
        at = i // 8 * (LANE // 4)
        return jnp.broadcast_to(recv_ref[:, i % 8, :][:, at : at + 1], (size, LANE))

    def over(x):
        return jnp.sum(x, axis=0, keepdims=True)

    (s, a, q, g, rr0, uu, uv, vv, ut, uw, vt, vw, bb, bv, bw, ww, bt, wt,
     ebb, ebv, ebw, evv, evw, eww) = [number(i) for i in range(24)]
    inv = 1.0 / s
    rr0 = over(rr0)
    curv0 = over(inv * (uv + a * vv))
    alpha0 = rr0 / curv0
    a0 = alpha0 * inv
    d = a - a0
    rr1 = over(uu + d * (2.0 * uv + d * vv))
    own1 = over(inv * (ut + d * (uw + q * uv + vt + d * (vw + q * vv))))
    cross1 = over(inv * (uv + d * vv))
    beta0 = rr1 / rr0
    curv1 = own1 + beta0 * (2.0 * cross1 + beta0 * curv0)
    alpha1 = rr1 / curv1
    a1 = alpha1 * inv
    c2 = a0 * a1
    m1 = g + c2
    m0 = a - a0 - a1 * (1.0 + beta0) + q * c2
    h = d * q + beta0
    rr2 = over(bb + m0 * (2.0 * bv + m0 * vv) + m1 * (2.0 * (bw + m0 * vw) + m1 * ww))
    cross2 = over(inv * (bt + d * bw + h * bv + m0 * (vt + d * vw + h * vv) + m1 * (wt + d * ww + h * vw)))
    own2 = over(ebb + m0 * (2.0 * ebv + m0 * evv) + m1 * (2.0 * (ebw + m0 * evw) + m1 * eww))
    beta1 = rr2 / rr1
    curv2 = own2 + beta1 * (2.0 * cross2 + beta1 * curv1)
    alpha2 = rr2 / curv2

    wide = lambda x: jnp.concatenate([x, x], axis=1)
    alpha0, alpha1, alpha2, beta0, beta1 = [wide(x) for x in (alpha0, alpha1, alpha2, beta0, beta1)]
    v0 = v0_ref[...]
    v1 = v1_ref[...]
    r1 = v0 - alpha0 * v1
    d1 = r1 + beta0 * v0
    image1 = (v1 - alpha0 * v2_ref[...]) + beta0 * v1
    r2 = r1 - alpha1 * image1
    d2 = r2 + beta1 * d1
    table_ref[...] = 0.5 * (alpha0 * v0 + alpha1 * d1 + alpha2 * d2)
    per = idx_ref.shape[0] // 2
    for j in range(per // 8):
        v = gather(table_ref, [idx_ref[k * per + j * 8 : k * per + j * 8 + 8, :] for k in range(2)], rows)
        for c in range(3):
            got = v[0][c] + v[1][c]
            for q in range(8):
                at = (j * 8 + q) * LANE
                out_ref[c : c + 1, at : at + LANE] = got[q : q + 1, :]


def call(kernel, args, outs, scratch=(), limit=None):
    spaces = {"s": pltpu.SMEM, "v": pltpu.VMEM, "h": pltpu.VMEM}
    arrays = [pltpu.with_memory_space_constraint(x, pltpu.VMEM) if m == "v" else x for x, m in args]
    return pl.pallas_call(
        kernel,
        out_shape=[o for o, _ in outs],
        in_specs=[pl.BlockSpec(memory_space=spaces[m]) for _, m in args],
        out_specs=[pl.BlockSpec(memory_space=spaces[m]) for _, m in outs],
        scratch_shapes=list(scratch),
        compiler_params=pltpu.CompilerParams(vmem_limit_bytes=limit),
    )(*arrays)


def rotated(x, axis, by):
    n = lax.axis_size(axis)
    return lax.ppermute(x, axis, [(i, (i + by) % n) for i in range(n)])


def traded(one, two):
    size = lax.axis_size("sub")
    groups = lax.axis_size("grp")
    outs = []
    for x, first in ((one, 0), (two, 1)):
        pairs = []
        for g in range(groups):
            for c in range(size):
                other = c + 1 if c % 2 == first else c - 1
                if 0 <= other < size:
                    pairs.append((g * size + c, g * size + other))
                else:
                    pairs.append((g * size + c, (g ^ 1) * size + c))
        outs.append(lax.ppermute(x, ("grp", "sub"), pairs))
    return outs


def body(fine_res, node_map, connect, grads, moduli, mass):
    size = lax.axis_size("sub")
    groups = lax.axis_size("grp")
    own = mass.shape[0]
    fine = node_map.shape[1]
    elems = connect.shape[1]
    rows = (own + CI) // LO
    k = CI // LO
    col = lax.axis_index("sub").astype(jnp.int32).reshape(1)
    fcount = 2 * fine // LANE
    ecount = 4 * elems // LANE

    def kept(*shape, dtype=jnp.float32):
        return pltpu.VMEM(shape, dtype), "v"

    table = kept(3 * HP, LO)
    edge = kept(3 * k, LO)
    acc = pltpu.VMEM((9 * HP, LO), jnp.float32)
    parts = pltpu.VMEM((9 * ecount, LANE), jnp.float32)
    strain = kept(6 * elems // LANE, LANE)
    mass2 = mass.reshape(own // LANE, LANE)

    partial, one, two, map_idx, mine = call(
        functools.partial(rhs_kernel, own=own),
        [(col, "s"), (node_map, "h"), (fine_res, "h"), (mass2, "h")],
        [table, kept(4 * k, LO), kept(4 * k, LO), kept(fcount, LANE, dtype=jnp.int32), kept(own // LO, LO)],
        [pltpu.VMEM((3 * fcount // 2, LANE), jnp.float32), pltpu.VMEM((LANE, fcount), jnp.float32),
         pltpu.VMEM((9 * fcount, LANE), jnp.float32), acc],
    )
    one, two = traded(one, two)
    idx, cols, g, mod = call(
        functools.partial(prep_kernel, own=own),
        [(col, "s"), (connect, "h"), (grads, "h"), (moduli, "h")],
        [kept(ecount, LANE, dtype=jnp.int32), kept(LANE, ecount), kept(9 * elems // LANE, LANE), kept(2 * elems // LANE, LANE)],
    )
    part, mass_ext = call(
        functools.partial(halo_kernel, own=own, size=size),
        [(col, "s"), (partial, "v"), (one, "v"), (two, "v"), (mine, "v"), (mod, "v")],
        [table, kept(HP, LO)],
    )
    sums = [part] + [rotated(part, "grp", i) for i in range(1, groups)]
    (hot,) = call(hot_kernel, [(cols, "v")], [kept(ecount * LANE, LO, dtype=jnp.bfloat16)], limit=ROOM)
    elements = [(idx, "v"), (g, "v"), (mod, "v")]
    summing = [(idx, "v"), (hot, "v"), (g, "v"), (mod, "v")]
    kw = dict(own=own, rows=rows)
    v0, f0, one, two, s0 = call(
        functools.partial(first_kernel, groups=groups, **kw),
        [(col, "s")] + [(x, "v") for x in sums] + summing,
        [table, table, edge, edge, strain],
        [parts, pltpu.VMEM((18 * HP, LO), jnp.float32)],
        ROOM,
    )
    one, two = traded(one, two)
    v1, f1, one, two, s1 = call(
        functools.partial(second_kernel, size=size, **kw),
        [(col, "s"), (one, "v"), (two, "v"), (v0, "v"), (f0, "v"), (mass_ext, "v")] + summing,
        [table, table, edge, edge, strain],
        [parts, pltpu.VMEM((18 * HP, LO), jnp.float32)],
        ROOM,
    )
    one, two = traded(one, two)
    msg, v2 = call(
        functools.partial(third_kernel, size=size, **kw),
        [(col, "s")] + [(x, "v") for x in (one, two, v0, v1, f1, s0, s1, mass_ext)] + elements,
        [kept(size, 8, LANE), table],
        [pltpu.VMEM((6 * elems // LANE, LANE), jnp.float32)],
    )
    recv = lax.all_to_all(msg, "sub", 0, 0)
    (out,) = call(
        functools.partial(last_kernel, rows=rows),
        [(recv, "v"), (v0, "v"), (v1, "v"), (v2, "v"), (map_idx, "v")],
        [(jax.ShapeDtypeStruct((3, fine), jnp.float32), "h")],
        [pltpu.VMEM((3 * HP, LO), jnp.float32)],
    )
    return out


def solution(mesh):
    in_specs = (
        P(None, ("grp", "sub")),
        P(None, ("grp", "sub")),
        P(None, "sub"),
        P(None, None, "sub"),
        P(None, "sub"),
        P("sub"),
    )
    out_specs = P(None, ("grp", "sub"))
    return jax.shard_map(body, mesh=mesh, in_specs=in_specs, out_specs=out_specs, check_vma=False)
```
